256 devices in a mesh: agent: 128 (over x, y, z), grid: 2 (over core).
Axes of the slice: x: 4, y: 4, z: 8, core: 2. Of those that a mesh axis runs over, the one named last changes fastest.
Arguments:
- value_prior: float32 [2048, 1024], P(None, 'agent'), may hold values from -6 to 6
- trans_weight: float32 [128, 128], replicated, may hold values from 0.05 to 1
- perceived_law_coefficient: float32 [4], replicated, may hold values from 0.7 to 1
- perceived_law_constant: float32 [4], replicated, may hold values from 0.5 to 4
- interest: float32 [4, 16], replicated, may hold values from 0 to 0.05
- wage_level: float32 [4, 16], replicated, may hold values from 0.5 to 1.5
- efficiency: float32 [32], replicated, may hold values from 0.2 to 3
- holdings: float32 [1048576], P('agent'), may hold values from 0 to 40
- shocks: int32 [4, 1048576], P(None, 'agent'), may hold values from 0 to 31
- brackets: int32 [4, 1048576], P(None, 'agent'), may hold values from 0 to 1022
- aggregate: int32 [4], replicated, may hold values from 0 to 3
Outputs:
- value_new: float32 [2048, 1024], P('agent', 'grid')
- policy: float32 [2048, 1024], P('agent', 'grid')
- holdings_final: float32 [1048576], P('agent')
- capital: float32 [4], replicated
The draws below stay inside these ranges and needn't reach their ends.
All inputs are finite; a program needn't handle non-finite values.
Results may differ from the reference program's by a relative error of at most 0.0003.
Values sent between devices are 32-bit elements; how exact they have to be, the bound alone decides.
A program may use at most 64 MiB of HBM per device.

```python
import math
import jax
import jax.numpy as jnp
from jax import lax

A = 1024
E = 32
NK = 16
Z = 4
STATES = 2048
AGENTS = 1048576
PERIODS = 4


wealth_upper_limit = 40.0


def bracket_start(key):
    base_key = jax.random.fold_in(key, 7)
    positions = jnp.arange(AGENTS, dtype=jnp.int32)
    stride = max(AGENTS // 1024, 1)
    buckets = (AGENTS + stride - 1) // stride
    bucket = positions // stride
    bracket_top = (A - 1) * 3 // 10 + bucket * ((A - 1) * 7 // 10) // buckets + 1
    return jax.random.randint(base_key, (AGENTS,), 0, bracket_top, dtype=jnp.int32)


def draw_brackets(key, part):
    first_row = bracket_start(key)
    later_rows = jax.random.randint(jax.random.fold_in(key, 9), (PERIODS - 1, AGENTS), 0, A - 1, dtype=jnp.int32)
    return jnp.concatenate([first_row[None, :], later_rows], axis=0)


def draw_holdings(key, part):
    start = bracket_start(key)
    fraction = jax.random.uniform(jax.random.fold_in(key, 11), (AGENTS,), jnp.float32, -0.25, 1.25)
    share_low = start.astype(jnp.float32) / (A - 1)
    share_high = (start + 1).astype(jnp.float32) / (A - 1)
    edge_low = wealth_upper_limit * share_low * share_low
    edge_high = wealth_upper_limit * share_high * share_high
    return jnp.clip(edge_low + fraction * (edge_high - edge_low), 0.0, wealth_upper_limit).astype(jnp.float32)


def place_ends(drawn, stream_key, low, largest):
    longest = drawn.shape.index(max(drawn.shape))
    spots = []
    for shift in (0, 1):
        where = [jax.random.randint(jax.random.fold_in(stream_key, axis), (), 0, length) for axis, length in enumerate(drawn.shape)]
        where[longest] = (where[longest] + shift) % drawn.shape[longest]
        spots.append(tuple(where))
    return drawn.at[spots[0]].set(low).at[spots[1]].set(largest)


def levels(stream_key, shape, cuts, low, largest):
    loudness = 1.0
    for axis_at, parts in cuts:
        steps = jax.random.uniform(jax.random.fold_in(jax.random.fold_in(stream_key, 6), axis_at), (parts,), jnp.float32, low / len(cuts), largest / len(cuts))
        loudness = loudness * jnp.repeat(jnp.exp(steps), shape[axis_at] // parts).reshape((-1,) + (1,) * (len(shape) - 1 - axis_at))
    return loudness


def centred(rng, extent, scale, reach, pieces=(), held_as=jnp.bfloat16):
    gain = levels(rng, extent, pieces, -0.22, 0.18) if pieces else 1.0
    values = jax.random.normal(rng, extent, jnp.float32) * scale * gain
    return jnp.minimum(jnp.maximum(values, -reach), reach).astype(held_as)


def setup_inputs(seed: int = 0) -> dict:
    splits = jax.random.split(jax.random.key(seed), 12)
    value_prior = centred(splits[0], (STATES, A), 1.0, 6.0, ((1, 128),), jnp.float32)
    trans_weight = jnp.clip(jnp.exp(jax.random.uniform(splits[1], (Z * E, Z * E), jnp.float32, math.log(0.05), math.log(1.0))), 0.05, 1.0)
    perceived_law_coefficient = jnp.clip(jnp.exp(jax.random.uniform(splits[2], (Z,), jnp.float32, math.log(0.7), math.log(1.0))), 0.7, 1.0)
    perceived_law_constant = jnp.clip(jax.random.uniform(splits[3], (Z,), jnp.float32, 0.5, 4.0), 0.5, 4.0)
    interest = jnp.clip(jax.random.uniform(splits[4], (Z, NK), jnp.float32, 0.0, 0.05), 0.0, 0.05)
    wage_level = jnp.clip(jax.random.uniform(splits[5], (Z, NK), jnp.float32, 0.5, 1.5), 0.5, 1.5)
    efficiency = jnp.clip(jnp.exp(jax.random.uniform(splits[6], (E,), jnp.float32, math.log(0.2), math.log(3.0))), 0.2, 3.0)
    holdings = draw_holdings(jax.random.fold_in(splits[11], 71), 0)
    shocks = place_ends(jax.random.randint(splits[8], (PERIODS, AGENTS), 0, E), jax.random.fold_in(splits[8], 1), 0, E - 1).astype(jnp.int32)
    brackets = draw_brackets(jax.random.fold_in(splits[11], 71), 0)
    aggregate = place_ends(jax.random.randint(splits[10], (PERIODS,), 0, Z), jax.random.fold_in(splits[10], 1), 0, Z - 1).astype(jnp.int32)
    return {"value_prior": value_prior, "trans_weight": trans_weight, "perceived_law_coefficient": perceived_law_coefficient, "perceived_law_constant": perceived_law_constant, "interest": interest, "wage_level": wage_level, "efficiency": efficiency, "holdings": holdings, "shocks": shocks, "brackets": brackets, "aggregate": aggregate}


wealth_upper_limit = 40.0
beta_disc = 0.96
tau_soft = 0.02
floor_cons = 0.1
highest = lax.Precision.HIGHEST


def make_points():
    fraction = jnp.arange(A, dtype=jnp.float32) / (A - 1)
    return wealth_upper_limit * fraction * fraction


def hat_function_shares(position):
    spacing = wealth_upper_limit / (NK - 1)
    savings_mesh_points = wealth_upper_limit * jnp.arange(NK, dtype=jnp.float32) / (NK - 1)
    return jnp.maximum(0.0, 1.0 - jnp.abs(position[..., None] - savings_mesh_points) / spacing)


def bellman(points, wealth, expected):
    consume = wealth[:, None] - points[None, :]
    clipped = jnp.maximum(consume, floor_cons)
    utility = jnp.log(clipped) + (consume - clipped) / floor_cons
    scores = (utility + beta_disc * expected[None, :]) / tau_soft
    highest_score = jnp.max(scores, axis=1, keepdims=True)
    weight = jnp.exp(scores - highest_score)
    totals = jnp.sum(weight, axis=1)
    values_now = tau_soft * (highest_score[:, 0] + jnp.log(totals))
    chosen = jnp.sum(weight * points[None, :], axis=1) / totals
    return values_now, chosen


def advance(lookup, points, current, shock_row, bracket_row):
    flattened = lookup.reshape(-1)
    flat_index = shock_row * lookup.shape[1] + bracket_row
    value_low = jnp.take(flattened, flat_index)
    value_high = jnp.take(flattened, flat_index + 1)
    edge_low = jnp.take(points, bracket_row)
    edge_high = jnp.take(points, bracket_row + 1)
    fraction = jnp.clip((current - edge_low) / (edge_high - edge_low), 0.0, 1.0)
    return value_low + fraction * (value_high - value_low)


def reference(value_prior, trans_weight, perceived_law_coefficient, perceived_law_constant, interest, wage_level, efficiency, holdings, shocks, brackets, aggregate):
    points = make_points()
    savings_mesh_points = wealth_upper_limit * jnp.arange(NK, dtype=jnp.float32) / (NK - 1)
    predicted_stock = jnp.clip(perceived_law_coefficient[:, None] * savings_mesh_points[None, :] + perceived_law_constant[:, None], 0.0, wealth_upper_limit)
    offset_coefficients = hat_function_shares(predicted_stock)
    transition = trans_weight / jnp.sum(trans_weight, axis=1, keepdims=True)
    value_cube = value_prior.reshape(Z, NK, E, A)
    mixed = jnp.einsum("ykfa,zjk->zjyfa", value_cube, offset_coefficients, precision=highest)
    expected = jnp.einsum("zjyfa,zeyf->zjea", mixed, transition.reshape(Z, E, Z, E), precision=highest).reshape(STATES, A)
    growth = jnp.broadcast_to((1.0 + interest)[:, :, None], (Z, NK, E)).reshape(STATES)
    income = (wage_level[:, :, None] * efficiency[None, None, :]).reshape(STATES)

    def one_state(packed):
        column, factor, earned = packed
        return bellman(points, points * factor + earned, column)

    values_now, policy = lax.map(one_state, (expected, growth, income))
    policy_cube = policy.reshape(Z, NK, E, A)
    current = holdings
    capital_path = []
    for period in range(PERIODS):
        capital = jnp.sum(current) / AGENTS
        capital_path.append(capital)
        sliced = lax.dynamic_index_in_dim(policy_cube, aggregate[period], 0, keepdims=False)
        lookup = jnp.einsum("k,kea->ea", hat_function_shares(capital), sliced, precision=highest)
        current = advance(lookup, points, current, shocks[period], brackets[period])
    return values_now, policy, current, jnp.stack(capital_path)
```

```python
import jax
import jax.numpy as jnp
from jax import lax
from jax.experimental import pallas as pl
from jax.experimental.pallas import tpu as pltpu
from jax.sharding import Mesh
from jax.sharding import PartitionSpec as P
MESH=pl.DeviceIdType.MESH
X,Y,ZC,G="agent_0","agent_1","agent_2","grid"
AGENT=(X,Y,ZC)
NK=16
f32=jnp.float32
i32=jnp.int32
LOG2E=1.4426950408889634
KT=500.0*LOG2E
SP=40.0/15
UN=32

def chip_id(a):
    return {X: a//32, Y: (a//8)%4, ZC: a%8}

def expect_kernel(vt_ref, tw_ref, coef_ref, const_ref, out_ref, send, recv, sem_s, sem_r):
    me=lax.axis_index(X)*32+lax.axis_index(Y)*8+lax.axis_index(ZC)
    bar=pltpu.get_barrier_semaphore()
    def sig(d,_):
        pl.semaphore_signal(bar,inc=1,device_id=chip_id(lax.rem(me+d,128)),device_id_type=MESH)
        return 0
    lax.fori_loop(1,128,sig,0)
    lane=lax.broadcasted_iota(jnp.int32,(8,128),1)
    sub=lax.broadcasted_iota(jnp.int32,(8,128),0)
    tw=tw_ref[...]
    tn=tw/jnp.sum(tw,axis=1,keepdims=True)
    blocks=[]
    for k in range(NK):
        b=None
        for y in range(4):
            col=(y*4+k//4)*128
            x=vt_ref[:,col:col+128]
            s=(y*32-(k%4)*32)%128
            if s: x=pltpu.roll(x,s,1)
            b=x if b is None else jnp.where(lane//32==y,x,b)
        blocks.append(b)
    vk=jnp.concatenate(blocks,axis=0)
    bl=lax.dot_general(vk,tn,(((1,),(1,)),((),())),precision=lax.Precision.HIGHEST,preferred_element_type=f32)
    zl=lane//32
    cf=jnp.where(zl==0,coef_ref[0],jnp.where(zl==1,coef_ref[1],jnp.where(zl==2,coef_ref[2],coef_ref[3])))
    cs=jnp.where(zl==0,const_ref[0],jnp.where(zl==1,const_ref[1],jnp.where(zl==2,const_ref[2],const_ref[3])))
    masks=[(lane//16-sub)%8==d for d in range(8)]
    for j in range(NK):
        fc=jnp.clip(cf*(40.0*j/15)+cs,0.0,40.0)
        acc=None
        for k in range(NK):
            h=jnp.maximum(0.0,1.0-jnp.abs(fc-(40.0*k/15))/SP)
            t=h*bl[k*8:k*8+8,:]
            acc=t if acc is None else acc+t
        o=acc
        for d in range(1,8):
            r=pltpu.roll(pltpu.roll(acc,(8-d)%8,0),16*d,1)
            o=jnp.where(masks[d],r,o)
        for g in range(8):
            send[j*8+g]=o[g:g+1,:]
    pl.semaphore_wait(bar,127)
    def row_of(a):
        return (a%32)//2*8+(a//32)*2+a%2
    def cp(d):
        a=lax.rem(me+d,128)
        return pltpu.make_async_remote_copy(src_ref=send.at[row_of(a)],dst_ref=recv.at[me],send_sem=sem_s,recv_sem=sem_r,device_id=chip_id(a),device_id_type=MESH)
    def go(d,_):
        cp(d).start()
        return 0
    lax.fori_loop(1,128,go,0)
    recv[me]=send[row_of(me)]
    pltpu.make_async_copy(recv.at[pl.ds(0,127)],recv.at[pl.ds(0,127)],sem_r).wait()
    for A in range(16):
        out_ref[A*8:A*8+8,:]=jnp.concatenate([recv[A*8+s] for s in range(8)],axis=0)
    pltpu.make_async_copy(send.at[pl.ds(0,127)],send.at[pl.ds(0,127)],sem_s).wait()

def expect(vt,tw,coef,const):
    vm=pl.BlockSpec(memory_space=pltpu.VMEM); sm=pl.BlockSpec(memory_space=pltpu.SMEM)
    return pl.pallas_call(expect_kernel,out_shape=jax.ShapeDtypeStruct((128,128),f32),
        in_specs=[vm,vm,sm,sm],out_specs=vm,
        scratch_shapes=[pltpu.VMEM((128,1,128),f32),pltpu.VMEM((128,1,128),f32),pltpu.SemaphoreType.DMA,pltpu.SemaphoreType.DMA],
        compiler_params=pltpu.CompilerParams(collective_id=0,has_side_effects=True),name="expect")(vt,tw,coef,const)


def hat(x,k):
    return jnp.maximum(0.0,1.0-jnp.abs(x-40.0*k/15)/SP)

def rdma(src,dst,ss,rs,**dev):
    return pltpu.make_async_remote_copy(src_ref=src,dst_ref=dst,send_sem=ss,recv_sem=rs,device_id=dev_ids(dev),device_id_type=MESH)
def dev_ids(dev):
    return {dict(x=X,y=Y,z=ZC,g=G)[k]:v for k,v in dev.items()}
def got(ref,sem):
    pltpu.make_async_copy(ref,ref,sem).wait()

def life(r_ref, hold_ref, shock_ref, brack_ref, int_ref, wage_ref, eff_ref, agg_ref,
         v_ref, p_ref, h_ref, cap_ref,
         pt,kpt,sc,rs,vb,pb,
         pxa,pxb,y0,z0,yb,lk,tt,oh,res,ri,li,pbk,inv,hp,hr,pay1,in1,pay2,in2,
         sx,rx,sy0,ry0,sz0,rz0,szt,rzt,sya,rya,syb,ryb,sh,rh,s1,r1,s2,r2):
    px=(pxa,pxb)
    x=lax.axis_index(X); y=lax.axis_index(Y); zc=lax.axis_index(ZC); g=lax.axis_index(G)
    bar=pltpu.get_barrier_semaphore()
    me_p=x*4+y
    me_l=zc*2+g
    def plane(d):
        o=lax.rem(me_p+d,16)
        return {X:o//4,Y:lax.rem(o,4)}
    def line(d):
        o=lax.rem(me_l+d,16)
        return {ZC:o//2,G:lax.rem(o,2)}
    def sig(d,_):
        pl.semaphore_signal(bar,inc=1,device_id=plane(d),device_id_type=MESH)
        pl.semaphore_signal(bar,inc=1,device_id=line(d),device_id_type=MESH)
        return 0
    lax.fori_loop(1,16,sig,0)

    def pts(A,_):
        for n in range(8):
            t=A*8+n
            j=(64*A+n+8*lax.broadcasted_iota(i32,(8,128),0)).astype(f32)
            fr=j/1023.0
            p=40.0*fr*fr
            o=pl.multiple_of(t*8,8)
            pt[pl.ds(o,8),:]=p
            kpt[pl.ds(o,8),:]=p*KT+0.1*KT
        return 0
    lax.fori_loop(0,16,pts,0)
    rs[...]=r_ref[...]*(48.0*LOG2E)
    k=y*4+zc//2
    eh=lax.rem(zc,2)
    growth=1.0+int_ref[x,k]
    wage=wage_ref[x,k]
    def state(e,_):
        inc=wage*eff_ref[eh*16+e]
        W=[];KW=[]
        for v in range(4):
            i=(lax.broadcasted_iota(i32,(8,128),1)+(128*v+512*g)).astype(f32)
            fr=i/1023.0
            w=(40.0*fr*fr)*growth+inc
            W.append(w);KW.append(w*KT)
        def p1(c,M):
            M=list(M)
            for u in range(UN):
                off=pl.multiple_of((c*UN+u)*8,8)
                P=pt[pl.ds(off,8),:]; KP=kpt[pl.ds(off,8),:]
                Rr=rs[pl.ds(pl.multiple_of((c*(UN//8)+u//8)*8,8),8),:]
                B=jnp.take_along_axis(Rr,jnp.full((8,128),(u%8)*16+e,i32),axis=1,mode="promise_in_bounds")
                D=B-KP
                for v in range(4):
                    cl=jnp.maximum(W[v]-P,0.1)
                    S=jnp.log(cl)*(50.0*LOG2E)+jnp.minimum(KW[v]+D,B)
                    sc[pl.ds(off,8),128*v:128*v+128]=S
                    M[v]=jnp.maximum(M[v],S)
            return tuple(M)
        M=lax.fori_loop(0,128//UN,p1,tuple(jnp.full((8,128),-1e30,f32) for _ in range(4)))
        def p2(c,acc):
            acc=list(acc)
            for u in range(UN):
                off=pl.multiple_of((c*UN+u)*8,8)
                P=pt[pl.ds(off,8),:]
                for v in range(4):
                    q=jnp.exp2(sc[pl.ds(off,8),128*v:128*v+128]-M[v])
                    acc[v]=acc[v]+q
                    acc[4+v]=acc[4+v]+P*q
            return tuple(acc)
        acc=lax.fori_loop(0,128//UN,p2,tuple(jnp.zeros((8,128),f32) for _ in range(8)))
        for v in range(4):
            m=jnp.max(M[v],axis=0,keepdims=True)
            s=jnp.exp2(M[v]-m)
            tot=jnp.sum(acc[v]*s,axis=0,keepdims=True)
            q=jnp.sum(acc[4+v]*s,axis=0,keepdims=True)
            vb[e,:,128*v:128*v+128]=jnp.broadcast_to((0.02/LOG2E)*m+0.02*jnp.log(tot),(8,128))
            pb[e,:,128*v:128*v+128]=jnp.broadcast_to(q/tot,(8,128))
        return 0
    def bell(a,b):
        lax.fori_loop(a,b,state,0)
    def finish(c):
        v_ref[c*8:c*8+8,:]=jnp.concatenate([vb[c*8+s,0:1,:] for s in range(8)],axis=0)
        p=jnp.concatenate([pb[c*8+s,0:1,:] for s in range(8)],axis=0)
        p_ref[c*8:c*8+8,:]=p
        px[c][x]=p

    def send_x(c):
        def go(d,_):
            rdma(px[c].at[x],px[c].at[x],sx.at[c],rx.at[c],x=lax.rem(x+d,4)).start()
            return 0
        lax.fori_loop(1,4,go,0)
    def send_y0(c,w):
        got(px[c].at[pl.ds(0,3)],rx.at[c])
        y0[c,y]=px[c][agg_ref[0]]*w
        def go(d,_):
            rdma(y0.at[c,y],y0.at[c,y],sy0.at[c],ry0.at[c],y=lax.rem(y+d,4)).start()
            return 0
        lax.fori_loop(1,4,go,0)
    def send_z0(c):
        got(y0.at[c,pl.ds(0,3)],ry0.at[c])
        z0[c,zc]=(y0[c,0]+y0[c,1])+(y0[c,2]+y0[c,3])
        def go(d,_):
            rdma(z0.at[c,zc],z0.at[c,zc],sz0.at[c],rz0.at[c],z=lax.rem(zc+d,8)).start()
            return 0
        lax.fori_loop(1,8,go,0)
    def table0(c):
        got(z0.at[c,pl.ds(0,7)],rz0.at[c])
        for h in range(2):
            lk[h*16+c*8:h*16+c*8+8,:]=(z0[c,h]+z0[c,2+h])+(z0[c,4+h]+z0[c,6+h])
    def send_slot(t):
        for c in range(2):
            yb[t-1,y,zc,c]=px[c][agg_ref[t]]
        def go(d,_):
            rdma(yb.at[t-1,y,zc],yb.at[t-1,y,zc],szt.at[t-1],rzt.at[t-1],z=lax.rem(zc+d,8)).start()
            return 0
        lax.fori_loop(1,8,go,0)
    up=lax.rem(y+1,4); down=lax.rem(y+3,4)
    def slot_a(t):
        got(yb.at[t-1,0,pl.ds(0,7)],rzt.at[t-1])
        for n,d in ((0,up),(1,down)):
            rdma(yb.at[t-1,y],yb.at[t-1,y],sya.at[t-1,n],rya.at[t-1,n],y=d).start()
    def slot_b(t):
        got(yb.at[t-1,0],rya.at[t-1,0])
        rdma(yb.at[t-1,down,pl.ds(0,4)],yb.at[t-1,down,pl.ds(0,4)],syb.at[t-1,0],ryb.at[t-1,0],y=up).start()
        got(yb.at[t-1,0],rya.at[t-1,1])
        rdma(yb.at[t-1,up,pl.ds(4,4)],yb.at[t-1,up,pl.ds(4,4)],syb.at[t-1,1],ryb.at[t-1,1],y=down).start()
    def slot_done(t):
        got(yb.at[t-1,0,pl.ds(0,4)],ryb.at[t-1,0])
        got(yb.at[t-1,0,pl.ds(0,4)],ryb.at[t-1,1])
    def table(t,cap):
        hs=[hat(cap,q) for q in range(16)]
        for h in range(2):
            for c in range(2):
                for v in range(4):
                    acc=None
                    for q in range(16):
                        w=hs[q]*yb[t-1,q//4,2*(q%4)+h,c,:,128*v:128*v+128]
                        acc=w if acc is None else acc+w
                    lk[h*16+c*8:h*16+c*8+8,128*v:128*v+128]=acc

    def sum_a(t,row):
        pay1[t]=row
        in1[t,me_l]=row
        def go(d,_):
            dv=line(d)
            pltpu.make_async_remote_copy(src_ref=pay1.at[t],dst_ref=in1.at[t,me_l],send_sem=s1.at[t],recv_sem=r1.at[t],device_id=dv,device_id_type=MESH).start()
            return 0
        lax.fori_loop(1,16,go,0)
    def total(buf,t):
        rows=[buf[t,n] for n in range(16)]
        while len(rows)>1:
            rows=[rows[2*n]+rows[2*n+1] for n in range(len(rows)//2)]
        return rows[0]
    def sum_b(t):
        got(in1.at[t,pl.ds(0,15)],r1.at[t])
        row=total(in1,t)
        pay2[t]=row
        in2[t,me_p]=row
        def go(d,_):
            dv=plane(d)
            pltpu.make_async_remote_copy(src_ref=pay2.at[t],dst_ref=in2.at[t,me_p],send_sem=s2.at[t],recv_sem=r2.at[t],device_id=dv,device_id_type=MESH).start()
            return 0
        lax.fori_loop(1,16,go,0)
    def sum_c(t):
        got(in2.at[t,pl.ds(0,15)],r2.at[t])
        cap=jnp.sum(total(in2,t))/1048576.0
        cap_ref[t]=cap
        return cap

    def index(n,_):
        cols=pl.ds(pl.multiple_of(n*1024,1024),1024)
        b=brack_ref[:,cols]; s=shock_ref[:,cols]
        edge=b==511
        own=(b//512)==g
        r=((b//128)%4)*32+s
        ri[:,cols]=jnp.where(own,r,jnp.where(jnp.logical_and(edge,g==1),s,-1))
        li[:,cols]=jnp.where(jnp.logical_and(edge,g==1),0,b%128)
        fa=b.astype(f32)/1023.0; fb=(b+1).astype(f32)/1023.0
        lo=40.0*fa*fa; hi=40.0*fb*fb
        pbk[:,cols]=lo
        inv[:,cols]=1.0/(hi-lo)
        return 0
    lane=lax.broadcasted_iota(i32,(32,128),1)
    iota=lax.broadcasted_iota(i32,(128,128),0)
    gf=g.astype(f32)
    def evolve(t):
        ls=[lk[:,128*v:128*v+128] for v in range(4)]
        ro=[pltpu.roll(q,127,1) for q in ls]
        ds=[]
        for v in range(4):
            nx=ro[v+1] if v<3 else ro[v]
            ds.append(jnp.where(lane==127,nx,ro[v])-ls[v])
        for o,q in ((0,ls),(128,ds)):
            m=jnp.concatenate(q,axis=0).T
            hi=m.astype(jnp.bfloat16)
            tt[o:o+128,0:128]=hi
            tt[o:o+128,128:256]=(m-hi.astype(f32)).astype(jnp.bfloat16)
        def grp(n,acc):
            base=n*1024
            for q in range(8):
                cols=pl.ds(pl.multiple_of(base+q*128,128),128)
                o=jnp.where(jnp.broadcast_to(ri[t:t+1,cols],(128,128))==iota,1.0,0.0).astype(jnp.bfloat16)
                oh[0:128,q*128:q*128+128]=o
                oh[128:256,q*128:q*128+128]=o
            res[...]=jnp.dot(tt[...],oh[...],preferred_element_type=f32)
            r8=pl.ds(pl.multiple_of(n*8,8),8)
            h=hold_ref[r8,:] if t==0 else hp[t-1,r8,:]+hr[t-1,r8,:]
            rows=[]
            for q in range(8):
                cols=pl.ds(pl.multiple_of(base+q*128,128),128)
                m=jnp.broadcast_to(li[t:t+1,cols],(128,128))==iota
                sl=jnp.sum(jnp.where(m,res[0:128,q*128:q*128+128],0.0),axis=0,keepdims=True)
                sd=jnp.sum(jnp.where(m,res[128:256,q*128:q*128+128],0.0),axis=0,keepdims=True)
                f=jnp.clip((h[q:q+1,:]-pbk[t:t+1,cols])*inv[t:t+1,cols],0.0,1.0)
                edge=brack_ref[t:t+1,cols]==511
                wl=jnp.where(edge,gf*f+(1.0-gf)*(1.0-f),1.0)
                wd=jnp.where(edge,0.0,f)
                rows.append(wl*sl+wd*sd)
            hn=jnp.concatenate(rows,axis=0)
            hp[t,r8,:]=hn
            return acc+hn
        acc=lax.fori_loop(0,8,grp,jnp.zeros((8,128),f32))
        rdma(hp.at[t],hr.at[t],sh.at[t],rh.at[t],g=1-g).start()
        return jnp.sum(acc,axis=0,keepdims=True)

    lax.fori_loop(0,8,index,0)
    h0=jnp.zeros((8,128),f32)
    for n in range(4):
        h0=h0+hold_ref[pl.ds(pl.multiple_of(g*32+n*8,8),8),:]
    pl.semaphore_wait(bar,30)
    sum_a(0,jnp.sum(h0,axis=0,keepdims=True))
    bell(0,4)
    sum_b(0)
    bell(4,8)
    finish(0)
    send_x(0)
    cap=sum_c(0)
    kf=k.astype(f32)
    w0=jnp.maximum(0.0,1.0-jnp.abs(cap-40.0*kf/15)/SP)
    bell(8,10)
    send_y0(0,w0)
    bell(10,12)
    send_z0(0)
    bell(12,16)
    finish(1)
    send_x(1)
    send_y0(1,w0)
    send_z0(1)
    for t in range(1,4):
        send_slot(t)
    table0(0)
    table0(1)
    for t in range(4):
        if t:
            slot_done(t)
            table(t,cap)
            got(hr.at[t-1],rh.at[t-1])
        row=evolve(t)
        if t<3:
            sum_a(t+1,row)
            if t==0:
                slot_a(1)
            sum_b(t+1)
            slot_b(t+1)
            if t<2:
                slot_a(t+2)
            cap=sum_c(t+1)
    got(hr.at[3],rh.at[3])
    h_ref[...]=hp[3]+hr[3]
    for c in range(2):
        got(px[c].at[pl.ds(0,3)],sx.at[c])
        got(y0.at[c,pl.ds(0,3)],sy0.at[c])
        got(z0.at[c,pl.ds(0,7)],sz0.at[c])
    for t in range(3):
        got(yb.at[t,0,pl.ds(0,7)],szt.at[t])
        for n in range(2):
            got(yb.at[t,0],sya.at[t,n])
            got(yb.at[t,0,pl.ds(0,4)],syb.at[t,n])
    for t in range(4):
        got(hp.at[t],sh.at[t])
        got(in1.at[t,pl.ds(0,15)],s1.at[t])
        got(in2.at[t,pl.ds(0,15)],s2.at[t])

def life_call(r,hold,shock,brack,interest,wage,eff,agg):
    vm=pl.BlockSpec(memory_space=pltpu.VMEM); sm=pl.BlockSpec(memory_space=pltpu.SMEM)
    V=lambda *s: pltpu.VMEM(s,f32)
    S=lambda *s: pltpu.SemaphoreType.DMA(s)
    return pl.pallas_call(life,
        out_shape=[jax.ShapeDtypeStruct((16,512),f32),jax.ShapeDtypeStruct((16,512),f32),jax.ShapeDtypeStruct((64,128),f32),jax.ShapeDtypeStruct((4,),f32)],
        in_specs=[vm]*4+[sm]*4,out_specs=[vm,vm,vm,sm],
        scratch_shapes=[V(1024,128),V(1024,128),V(1024,512),V(128,128),V(16,8,512),V(16,8,512),
            V(4,8,512),V(4,8,512),V(2,4,8,512),V(2,8,8,512),V(3,4,8,2,8,512),V(32,512),pltpu.VMEM((256,256),jnp.bfloat16),pltpu.VMEM((256,1024),jnp.bfloat16),V(256,1024),
            pltpu.VMEM((4,8192),i32),pltpu.VMEM((4,8192),i32),V(4,8192),V(4,8192),V(4,64,128),V(4,64,128),V(4,1,128),V(4,16,1,128),V(4,1,128),V(4,16,1,128),
            S(2),S(2),S(2),S(2),S(2),S(2),S(3),S(3),S(3,2),S(3,2),S(3,2),S(3,2),S(4),S(4),S(4),S(4),S(4),S(4)],
        compiler_params=pltpu.CompilerParams(collective_id=1,has_side_effects=True,vmem_limit_bytes=40*1024*1024),name="life")(r,hold,shock,brack,interest,wage,eff,agg)


def on_device(value_prior,trans_weight,coefficient,constant,interest,wage_level,efficiency,holdings,shocks,brackets,aggregate):
    arrived=expect(value_prior.T,trans_weight,coefficient,constant)
    values_now,policy,final,capital=life_call(arrived,holdings.reshape(64,128),shocks,brackets,interest,wage_level,efficiency,aggregate)
    return values_now,policy,final.reshape(8192),capital


def solution(mesh):
    finer=Mesh(mesh.devices.reshape(4,4,8,mesh.shape["grid"]),(X,Y,ZC,G))
    in_specs=(P(None,AGENT),P(),P(),P(),P(),P(),P(),P(AGENT),P(None,AGENT),P(None,AGENT),P())
    out_specs=(P(AGENT,G),P(AGENT,G),P(AGENT),P())
    return jax.shard_map(on_device,mesh=finer,in_specs=in_specs,out_specs=out_specs,check_vma=False)
```

```python
import jax
import jax.numpy as jnp
from jax import lax
from jax.experimental import pallas as pl
from jax.experimental.pallas import tpu as pltpu
from jax.sharding import Mesh
from jax.sharding import PartitionSpec as P
MESH=pl.DeviceIdType.MESH
X,Y,ZC,G="agent_0","agent_1","agent_2","grid"
AGENT=(X,Y,ZC)
f32=jnp.float32
i32=jnp.int32
LOG2E=1.4426950408889634
KT=500.0*LOG2E
SP=40.0/15
UN=32

def hat(x,k):
    return jnp.maximum(0.0,1.0-jnp.abs(x-40.0*k/15)/SP)

def rdma(src,dst,ss,rs,**dev):
    return pltpu.make_async_remote_copy(src_ref=src,dst_ref=dst,send_sem=ss,recv_sem=rs,device_id=dev_ids(dev),device_id_type=MESH)
def dev_ids(dev):
    return {dict(x=X,y=Y,z=ZC,g=G)[k]:v for k,v in dev.items()}
def got(ref,sem):
    pltpu.make_async_copy(ref,ref,sem).wait()


CH=((0,8),(8,4),(12,4))

def life(vt_hbm, tw_hbm, hold_hbm, shock_hbm, brack_hbm, coef_ref, const_ref, int_ref, wage_ref, eff_ref, agg_ref,
         v_ref, p_ref, h_ref, cap_ref,
         vt_ref,tw_ref,hold_ref,shock_ref,brack_ref,send,mid,recv,
         pt,kpt,sc,rs,vb,pb,
         pxa,pxb,pxc,y0a,y0b,y0c,z0a,z0b,z0c,yba,ybb,lk,tt,oh,resa,resb,ri,li,own,pbk,inv,fr_s,hp,hr,pay1,in1,pay2,in2,wt,cl,ctot,
         sin,sa1,ra1,sa2,ra2,sx,rx,sy0,ry0,sz0,rz0,szt,rzt,sya,rya,syb,ryb,sh,rh,s1,r1,s2,r2):
    px=(pxa,pxb,pxc); y0=(y0a,y0b,y0c); z0=(z0a,z0b,z0c); yb=(yba,ybb); res=(resa,resb)
    x=lax.axis_index(X); y=lax.axis_index(Y); zc=lax.axis_index(ZC); g=lax.axis_index(G)
    inputs=[pltpu.make_async_copy(a,b,sin.at[n]) for n,(a,b) in enumerate(((vt_hbm,vt_ref),(tw_hbm,tw_ref),(hold_hbm,hold_ref),(shock_hbm,shock_ref),(brack_hbm,brack_ref)))]
    for c in inputs:
        c.start()
    bar=pltpu.get_barrier_semaphore()
    me_p=x*4+y
    me_l=zc*2+g
    def plane(d):
        o=lax.rem(me_p+d,16)
        return {X:o//4,Y:lax.rem(o,4)}
    def line(d):
        o=lax.rem(me_l+d,16)
        return {ZC:o//2,G:lax.rem(o,2)}
    def sig(d,_):
        pl.semaphore_signal(bar,inc=1,device_id=plane(d),device_id_type=MESH)
        pl.semaphore_signal(bar,inc=1,device_id=line(d),device_id_type=MESH)
        return 0
    lax.fori_loop(1,16,sig,0)

    lane8=lax.broadcasted_iota(i32,(8,128),1)
    sub8=lax.broadcasted_iota(i32,(8,128),0)
    def expect():
        inputs[0].wait(); inputs[1].wait()
        tw=tw_ref[...]
        tn=tw/jnp.sum(tw,axis=1,keepdims=True)
        blocks=[]
        for k in range(16):
            b=None
            for q in range(4):
                col=(q*4+k//4)*128
                w=vt_ref[:,col:col+128]
                d=(q*32-(k%4)*32)%128
                if d: w=pltpu.roll(w,d,1)
                b=w if b is None else jnp.where(lane8//32==q,w,b)
            blocks.append(b)
        vk=jnp.concatenate(blocks,axis=0)
        bl=lax.dot_general(vk,tn,(((1,),(1,)),((),())),precision=lax.Precision.HIGHEST,preferred_element_type=f32)
        zl=lane8//32
        def per_zone(r):
            return jnp.where(zl==0,r[0],jnp.where(zl==1,r[1],jnp.where(zl==2,r[2],r[3])))
        cf=per_zone(coef_ref); cs=per_zone(const_ref)
        masks=[(lane8//16-sub8)%8==d for d in range(8)]
        for j in range(16):
            fc=jnp.clip(cf*(40.0*j/15)+cs,0.0,40.0)
            acc=None
            for k in range(16):
                w=hat(fc,k)*bl[k*8:k*8+8,:]
                acc=w if acc is None else acc+w
            o=acc
            for d in range(1,8):
                o=jnp.where(masks[d],pltpu.roll(pltpu.roll(acc,8-d,0),16*d,1),o)
            for q in range(8):
                send[(j%4)*2+q%2,(q//2)*4+j//4]=o[q:q+1,:]
    def expect_a():
        def go(d,_):
            o=lax.rem(zc+d,8)
            rdma(send.at[o],mid.at[zc],sa1,ra1,z=o).start()
            return 0
        lax.fori_loop(1,8,go,0)
        mid[zc]=send[zc]
    def expect_b():
        got(mid.at[pl.ds(0,7)],ra1)
        def go(d,_):
            o=lax.rem(me_p+d,16)
            rdma(mid.at[:,o],recv.at[me_p],sa2,ra2,x=o//4,y=lax.rem(o,4)).start()
            return 0
        lax.fori_loop(1,16,go,0)
        recv[me_p]=mid[:,me_p]
    def expect_c():
        got(recv.at[pl.ds(0,15)],ra2)
        for q in range(16):
            rs[q*8:q*8+8,:]=jnp.concatenate([recv[q,n] for n in range(8)],axis=0)*(48.0*LOG2E)

    def pts(A,_):
        for n in range(8):
            t=A*8+n
            j=(64*A+n+8*sub8).astype(f32)
            fr=j/1023.0
            p=40.0*fr*fr
            o=pl.multiple_of(t*8,8)
            pt[pl.ds(o,8),:]=p
            kpt[pl.ds(o,8),:]=p*KT+0.1*KT
        return 0
    k=y*4+zc//2
    eh=lax.rem(zc,2)
    growth=1.0+int_ref[x,k]
    wage=wage_ref[x,k]
    def state(e,_):
        inc=wage*eff_ref[eh*16+e]
        W=[];KW=[]
        for v in range(4):
            i=(lax.broadcasted_iota(i32,(8,128),1)+(128*v+512*g)).astype(f32)
            fr=i/1023.0
            w=(40.0*fr*fr)*growth+inc
            W.append(w);KW.append(w*KT)
        def p1(c,M):
            M=list(M)
            for u in range(UN):
                off=pl.multiple_of((c*UN+u)*8,8)
                P=pt[pl.ds(off,8),:]; KP=kpt[pl.ds(off,8),:]
                Rr=rs[pl.ds(pl.multiple_of((c*(UN//8)+u//8)*8,8),8),:]
                B=jnp.take_along_axis(Rr,jnp.full((8,128),(u%8)*16+e,i32),axis=1,mode="promise_in_bounds")
                D=B-KP
                for v in range(4):
                    cl=jnp.maximum(W[v]-P,0.1)
                    S=jnp.log(cl)*(50.0*LOG2E)+jnp.minimum(KW[v]+D,B)
                    sc[pl.ds(off,8),128*v:128*v+128]=S
                    M[v]=jnp.maximum(M[v],S)
            return tuple(M)
        M=lax.fori_loop(0,128//UN,p1,tuple(jnp.full((8,128),-1e30,f32) for _ in range(4)))
        def p2(c,acc):
            acc=list(acc)
            for u in range(UN):
                off=pl.multiple_of((c*UN+u)*8,8)
                P=pt[pl.ds(off,8),:]
                for v in range(4):
                    q=jnp.exp2(sc[pl.ds(off,8),128*v:128*v+128]-M[v])
                    acc[v]=acc[v]+q
                    acc[4+v]=acc[4+v]+P*q
            return tuple(acc)
        acc=lax.fori_loop(0,128//UN,p2,tuple(jnp.zeros((8,128),f32) for _ in range(8)))
        for v in range(4):
            m=jnp.max(M[v],axis=0,keepdims=True)
            s=jnp.exp2(M[v]-m)
            tot=jnp.sum(acc[v]*s,axis=0,keepdims=True)
            q=jnp.sum(acc[4+v]*s,axis=0,keepdims=True)
            vb[e,:,128*v:128*v+128]=jnp.broadcast_to((0.02/LOG2E)*m+0.02*jnp.log(tot),(8,128))
            pb[e,:,128*v:128*v+128]=jnp.broadcast_to(q/tot,(8,128))
        return 0
    def bell(a,b):
        lax.fori_loop(a,b,state,0)
    def finish(c):
        a,n=CH[c]
        v_ref[a:a+n,:]=jnp.concatenate([vb[a+q,0:1,:] for q in range(n)],axis=0)
        p=jnp.concatenate([pb[a+q,0:1,:] for q in range(n)],axis=0)
        p_ref[a:a+n,:]=p
        px[c][x]=p

    def send_x(c):
        def go(d,_):
            rdma(px[c].at[x],px[c].at[x],sx.at[c],rx.at[c],x=lax.rem(x+d,4)).start()
            return 0
        lax.fori_loop(1,4,go,0)
    def send_y0(c,w):
        got(px[c].at[pl.ds(0,3)],rx.at[c])
        y0[c][y]=px[c][agg_ref[0]]*w
        def go(d,_):
            rdma(y0[c].at[y],y0[c].at[y],sy0.at[c],ry0.at[c],y=lax.rem(y+d,4)).start()
            return 0
        lax.fori_loop(1,4,go,0)
    def send_z0(c):
        got(y0[c].at[pl.ds(0,3)],ry0.at[c])
        b=y0[c]
        z0[c][zc]=(b[0]+b[1])+(b[2]+b[3])
        def go(d,_):
            rdma(z0[c].at[zc],z0[c].at[zc],sz0.at[c],rz0.at[c],z=lax.rem(zc+d,8)).start()
            return 0
        lax.fori_loop(1,8,go,0)
    def table0(c):
        got(z0[c].at[pl.ds(0,7)],rz0.at[c])
        a,n=CH[c]
        b=z0[c]
        for h in range(2):
            lk[h*16+a:h*16+a+n,:]=(b[h]+b[2+h])+(b[4+h]+b[6+h])
    def send_slot(t,half):
        b=yb[half]
        if half==0:
            b[t-1,y,zc]=px[0][agg_ref[t]]
        else:
            b[t-1,y,zc,0:4]=px[1][agg_ref[t]]
            b[t-1,y,zc,4:8]=px[2][agg_ref[t]]
        def go(d,_):
            rdma(b.at[t-1,y,zc],b.at[t-1,y,zc],szt.at[t-1,half],rzt.at[t-1,half],z=lax.rem(zc+d,8)).start()
            return 0
        lax.fori_loop(1,8,go,0)
    up=lax.rem(y+1,4); down=lax.rem(y+3,4)
    def slot_a(t,half):
        b=yb[half]
        got(b.at[t-1,0,pl.ds(0,7)],rzt.at[t-1,half])
        for n,d in ((0,up),(1,down)):
            rdma(b.at[t-1,y],b.at[t-1,y],sya.at[t-1,half,n],rya.at[t-1,half,n],y=d).start()
    def slot_b(t,half):
        b=yb[half]
        got(b.at[t-1,0],rya.at[t-1,half,0])
        rdma(b.at[t-1,down,pl.ds(0,4)],b.at[t-1,down,pl.ds(0,4)],syb.at[t-1,half,0],ryb.at[t-1,half,0],y=up).start()
        got(b.at[t-1,0],rya.at[t-1,half,1])
        rdma(b.at[t-1,up,pl.ds(4,4)],b.at[t-1,up,pl.ds(4,4)],syb.at[t-1,half,1],ryb.at[t-1,half,1],y=down).start()
    def slot_done(t):
        for half in range(2):
            b=yb[half]
            got(b.at[t-1,0,pl.ds(0,4)],ryb.at[t-1,half,0])
            got(b.at[t-1,0,pl.ds(0,4)],ryb.at[t-1,half,1])
    def table(t,cap):
        hs=[hat(cap,q) for q in range(16)]
        for h in range(2):
            for c in range(2):
                for v in range(4):
                    acc=None
                    for q in range(16):
                        w=hs[q]*yb[c][t-1,q//4,2*(q%4)+h,:,128*v:128*v+128]
                        acc=w if acc is None else acc+w
                    lk[h*16+c*8:h*16+c*8+8,128*v:128*v+128]=acc

    def sum_a(t,row):
        pay1[t]=row
        in1[t,me_l]=row
        def go(d,_):
            pltpu.make_async_remote_copy(src_ref=pay1.at[t],dst_ref=in1.at[t,me_l],send_sem=s1.at[t],recv_sem=r1.at[t],device_id=line(d),device_id_type=MESH).start()
            return 0
        lax.fori_loop(1,16,go,0)
    def total(buf,t):
        rows=[buf[t,n] for n in range(16)]
        while len(rows)>1:
            rows=[rows[2*n]+rows[2*n+1] for n in range(len(rows)//2)]
        return rows[0]
    def sum_b(t):
        got(in1.at[t,pl.ds(0,15)],r1.at[t])
        row=total(in1,t)
        pay2[t]=row
        in2[t,me_p]=row
        def go(d,_):
            pltpu.make_async_remote_copy(src_ref=pay2.at[t],dst_ref=in2.at[t,me_p],send_sem=s2.at[t],recv_sem=r2.at[t],device_id=plane(d),device_id_type=MESH).start()
            return 0
        lax.fori_loop(1,16,go,0)
    def sum_c(t):
        got(in2.at[t,pl.ds(0,15)],r2.at[t])
        return total(in2,t)
    def mean_of(t,row):
        cap=jnp.sum(row)/1048576.0
        cap_ref[t]=cap
        return cap

    def index(n,_):
        cols=pl.ds(pl.multiple_of(n*1024,1024),1024)
        b=brack_ref[:,cols]; e=shock_ref[:,cols]
        edge=jnp.logical_and(b==511,g==1)
        mine=(b//512)==g
        r=((b//128)%4)*32+e
        ri[:,cols]=jnp.where(mine,r,jnp.where(edge,96+e,-1))
        li[:,cols]=jnp.where(edge,127,b%128)
        own[:,cols]=jnp.where(edge,0.0,1.0)
        fa=b.astype(f32)/1023.0; fb=(b+1).astype(f32)/1023.0
        lo=40.0*fa*fa; hi=40.0*fb*fb
        pbk[:,cols]=lo
        inv[:,cols]=1.0/(hi-lo)
        return 0
    lane=lax.broadcasted_iota(i32,(32,128),1)
    iota=lax.broadcasted_iota(i32,(128,128),0)
    def hot(t):
        def go(n,_):
            for q in range(8):
                cols=pl.ds(pl.multiple_of(n*1024+q*128,128),128)
                o=jnp.where(jnp.broadcast_to(ri[t:t+1,cols],(128,128))==iota,1.0,0.0).astype(jnp.bfloat16)
                oh[t,0:128,cols]=o
                oh[t,128:256,cols]=o
            return 0
        lax.fori_loop(0,8,go,0)
    def shares(t):
        for n in range(8):
            r8=slice(n*8,n*8+8)
            h=hold_ref[r8,:] if t==0 else hp[t-1,r8,:]+hr[t-1,r8,:]
            for q in range(8):
                cols=slice((n*8+q)*128,(n*8+q)*128+128)
                fr_s[t:t+1,cols]=jnp.clip((h[q:q+1,:]-pbk[t:t+1,cols])*inv[t:t+1,cols],0.0,1.0)
    def evolve(t):
        ls=[lk[:,128*v:128*v+128] for v in range(4)]
        ro=[pltpu.roll(q,127,1) for q in ls]
        ds=[jnp.where(lane==127,ro[v+1],ro[v])-ls[v] for v in range(3)]
        last=jnp.where(g==1,ro[0],-ls[3])
        first=jnp.broadcast_to(ls[0][:,0:1],(32,128))
        last=jnp.where(g==1,first,-ls[3])
        ds.append(jnp.where(lane==127,last,ro[3]-ls[3]))
        for o,q in ((0,ls),(128,ds)):
            m=jnp.concatenate(q,axis=0).T
            hi=m.astype(jnp.bfloat16)
            tt[o:o+128,0:128]=hi
            tt[o:o+128,128:256]=(m-hi.astype(f32)).astype(jnp.bfloat16)
        acc=None
        table_now=tt[...]
        for n in range(8):
            rb=res[n%2]
            rb[...]=jnp.dot(table_now,oh[t,:,n*1024:n*1024+1024],preferred_element_type=f32)
            rows=[]
            for q in range(8):
                cols=slice(n*1024+q*128,n*1024+q*128+128)
                m=jnp.broadcast_to(li[t:t+1,cols],(128,128))==iota
                sl=jnp.sum(jnp.where(m,rb[0:128,q*128:q*128+128],0.0),axis=0,keepdims=True)
                sd=jnp.sum(jnp.where(m,rb[128:256,q*128:q*128+128],0.0),axis=0,keepdims=True)
                rows.append(own[t:t+1,cols]*sl+fr_s[t:t+1,cols]*sd)
            hn=jnp.concatenate(rows,axis=0)
            hp[t,n*8:n*8+8,:]=hn
            acc=hn if acc is None else acc+hn
        rdma(hp.at[t],hr.at[t],sh.at[t],rh.at[t],g=1-g).start()
        return jnp.sum(acc,axis=0,keepdims=True)
    def counts(t):
        acc=None
        for n in range(8):
            for q in range(8):
                cols=slice(n*1024+q*128,n*1024+q*128+128)
                m=jnp.broadcast_to(li[t:t+1,cols],(128,128))==iota
                wt[0:128,q*128:q*128+128]=jnp.where(m,jnp.broadcast_to(own[t:t+1,cols],(128,128)),0.0).astype(jnp.bfloat16)
            d=lax.dot_general(oh[t,0:128,n*1024:n*1024+1024],wt[0:128,:],(((1,),(1,)),((),())),preferred_element_type=f32)
            acc=d if acc is None else acc+d
        cl[...]=acc
    def weights(t):
        acc=None
        for n in range(8):
            for q in range(8):
                cols=slice(n*1024+q*128,n*1024+q*128+128)
                m=jnp.broadcast_to(li[t:t+1,cols],(128,128))==iota
                f=jnp.broadcast_to(fr_s[t:t+1,cols],(128,128))
                hi=f.astype(jnp.bfloat16).astype(f32)
                wt[0:128,q*128:q*128+128]=jnp.where(m,hi,0.0).astype(jnp.bfloat16)
                wt[128:256,q*128:q*128+128]=jnp.where(m,f-hi,0.0).astype(jnp.bfloat16)
            d=lax.dot_general(oh[t,0:128,n*1024:n*1024+1024],wt[...],(((1,),(1,)),((),())),preferred_element_type=f32)
            acc=d if acc is None else acc+d
        cd=acc[:,0:128]+acc[:,128:256]
        cs=[cd[32*v:32*v+32,:] for v in range(4)]
        ro=[pltpu.roll(q,1,1) for q in cs]
        for v in range(4):
            if v==3:
                inner=jnp.where(lane==127,0.0,cs[3])
                ctot_v=cl[96:128,:]-inner
                ctot_v=ctot_v-jnp.where(jnp.logical_and(lane==127,g==0),cs[3],0.0)
            else:
                ctot_v=cl[32*v:32*v+32,:]-cs[v]
            prev=ro[v-1] if v else jnp.where(g==1,ro[3],jnp.zeros_like(ro[3]))
            ctot[:,128*v:128*v+128]=ctot_v+jnp.where(lane==0,prev,ro[v])
    lane1=lax.broadcasted_iota(i32,(1,128),1)
    def moments(t,row):
        out=jnp.where(lane1==16,jnp.sum(row,axis=1,keepdims=True),0.0)
        for q in range(16):
            acc=None
            for h in range(2):
                for c in range(2):
                    for v in range(4):
                        w=ctot[h*16+c*8:h*16+c*8+8,128*v:128*v+128]*yb[c][t-1,q//4,2*(q%4)+h,:,128*v:128*v+128]
                        acc=w if acc is None else acc+w
            m=jnp.sum(jnp.sum(acc,axis=0,keepdims=True),axis=1,keepdims=True)
            out=jnp.where(lane1==q,m,out)
        return out

    lax.fori_loop(0,16,pts,0)
    expect()
    for c in inputs[2:]:
        c.wait()
    lax.fori_loop(0,8,index,0)
    h0=jnp.zeros((8,128),f32)
    for n in range(4):
        h0=h0+hold_ref[pl.ds(pl.multiple_of(g*32+n*8,8),8),:]
    pl.semaphore_wait(bar,30)
    expect_a()
    sum_a(0,jnp.sum(h0,axis=0,keepdims=True))
    shares(0)
    hot(0)
    expect_b()
    sum_b(0)
    hot(1)
    hot(2)
    counts(2)
    expect_c()
    bell(0,6)
    row=sum_c(0)
    cap=mean_of(0,row)
    kf=k.astype(f32)
    w0=jnp.maximum(0.0,1.0-jnp.abs(cap-40.0*kf/15)/SP)
    bell(6,8)
    finish(0)
    send_x(0)
    bell(8,10)
    send_y0(0,w0)
    send_slot(1,0)
    bell(10,12)
    finish(1)
    send_x(1)
    send_z0(0)
    send_slot(2,0)
    bell(12,14)
    send_y0(1,w0)
    slot_a(1,0)
    bell(14,16)
    finish(2)
    send_x(2)
    send_z0(1)
    slot_b(1,0)
    send_y0(2,w0)
    send_z0(2)
    send_slot(1,1)
    send_slot(2,1)
    send_slot(3,0)
    send_slot(3,1)
    slot_a(2,0)
    table0(0)
    table0(1)
    table0(2)
    row=evolve(0)
    sum_a(1,row)
    slot_a(1,1)
    slot_b(2,0)
    sum_b(1)
    slot_b(1,1)
    slot_a(2,1)
    slot_a(3,0)
    got(hr.at[0],rh.at[0])
    shares(1)
    hot(3)
    cap=mean_of(1,sum_c(1))
    slot_done(1)
    table(1,cap)
    row=evolve(1)
    slot_b(2,1)
    slot_b(3,0)
    slot_a(3,1)
    got(hr.at[1],rh.at[1])
    shares(2)
    weights(2)
    slot_done(2)
    sum_a(2,moments(2,row))
    sum_b(2)
    slot_b(3,1)
    row=sum_c(2)
    cap=jnp.sum(jnp.where(lane1==16,row,0.0))/1048576.0
    cap_ref[2]=cap
    table(2,cap)
    qs=lane1.astype(f32)*40.0/15
    cap3=jnp.sum(jnp.where(lane1<16,jnp.maximum(0.0,1.0-jnp.abs(cap-qs)/SP)*row,0.0))/1048576.0
    cap_ref[3]=cap3
    evolve(2)
    slot_done(3)
    table(3,cap3)
    got(hr.at[2],rh.at[2])
    shares(3)
    evolve(3)
    got(hr.at[3],rh.at[3])
    h_ref[...]=hp[3]+hr[3]
    got(mid.at[pl.ds(0,7)],sa1)
    got(recv.at[pl.ds(0,15)],sa2)
    for c in range(3):
        got(px[c].at[pl.ds(0,3)],sx.at[c])
        got(y0[c].at[pl.ds(0,3)],sy0.at[c])
        got(z0[c].at[pl.ds(0,7)],sz0.at[c])
    for t in range(3):
        for half in range(2):
            b=yb[half]
            got(b.at[t,0,pl.ds(0,7)],szt.at[t,half])
            for n in range(2):
                got(b.at[t,0],sya.at[t,half,n])
                got(b.at[t,0,pl.ds(0,4)],syb.at[t,half,n])
    for t in range(4):
        got(hp.at[t],sh.at[t])
    for t in range(3):
        got(in1.at[t,pl.ds(0,15)],s1.at[t])
        got(in2.at[t,pl.ds(0,15)],s2.at[t])

def life_call(vt,tw,hold,shock,brack,coef,const,interest,wage,eff,agg):
    vm=pl.BlockSpec(memory_space=pltpu.VMEM); sm=pl.BlockSpec(memory_space=pltpu.SMEM); hb=pl.BlockSpec(memory_space=pl.ANY)
    V=lambda *s: pltpu.VMEM(s,f32)
    B=lambda *s: pltpu.VMEM(s,jnp.bfloat16)
    I=lambda *s: pltpu.VMEM(s,i32)
    S=lambda *s: pltpu.SemaphoreType.DMA(s)
    one=pltpu.SemaphoreType.DMA
    return pl.pallas_call(life,
        out_shape=[jax.ShapeDtypeStruct((16,512),f32),jax.ShapeDtypeStruct((16,512),f32),jax.ShapeDtypeStruct((64,128),f32),jax.ShapeDtypeStruct((4,),f32)],
        in_specs=[hb]*5+[sm]*6,out_specs=[vm,vm,vm,sm],
        scratch_shapes=[V(8,2048),V(128,128),V(64,128),I(4,8192),I(4,8192),V(8,16,1,128),V(8,16,1,128),V(16,8,1,128),
            V(1024,128),V(1024,128),V(1024,512),V(128,128),V(16,8,512),V(16,8,512),
            V(4,8,512),V(4,4,512),V(4,4,512),V(4,8,512),V(4,4,512),V(4,4,512),V(8,8,512),V(8,4,512),V(8,4,512),
            V(3,4,8,8,512),V(3,4,8,8,512),V(32,512),B(256,256),B(4,256,8192),V(256,1024),V(256,1024),
            I(4,8192),I(4,8192),V(4,8192),V(4,8192),V(4,8192),V(4,8192),V(4,64,128),V(4,64,128),V(3,1,128),V(3,16,1,128),V(3,1,128),V(3,16,1,128),
            B(256,1024),V(128,128),V(32,512),
            S(5),one,one,one,one,S(3),S(3),S(3),S(3),S(3),S(3),S(3,2),S(3,2),S(3,2,2),S(3,2,2),S(3,2,2),S(3,2,2),S(4),S(4),S(3),S(3),S(3),S(3)],
        compiler_params=pltpu.CompilerParams(collective_id=1,has_side_effects=True,vmem_limit_bytes=56*1024*1024),name="life")(vt,tw,hold,shock,brack,coef,const,interest,wage,eff,agg)

def put_out(v,p,h,c,vo,po,ho,co,sem):
    copies=[pltpu.make_async_copy(a,b,sem.at[n]) for n,(a,b) in enumerate(((v,vo),(p,po),(h,ho)))]
    for q in copies:
        q.start()
    for n in range(4):
        co[n]=c[n]
    for q in copies:
        q.wait()

def put_out_call(v,p,h,c):
    vm=pl.BlockSpec(memory_space=pltpu.VMEM); sm=pl.BlockSpec(memory_space=pltpu.SMEM); hb=pl.BlockSpec(memory_space=pl.ANY)
    return pl.pallas_call(put_out,out_shape=[jax.ShapeDtypeStruct(a.shape,f32) for a in (v,p,h,c)],in_specs=[vm,vm,vm,sm],out_specs=[hb,hb,hb,sm],
        scratch_shapes=[pltpu.SemaphoreType.DMA((3,))],name="put_out")(v,p,h,c)


def on_device(value_prior,trans_weight,coefficient,constant,interest,wage_level,efficiency,holdings,shocks,brackets,aggregate):
    values_now,policy,final,capital=life_call(value_prior.T,trans_weight,holdings.reshape(64,128),shocks,brackets,coefficient,constant,interest,wage_level,efficiency,aggregate)
    values_now,policy,final,capital=put_out_call(values_now,policy,final,capital)
    return values_now,policy,final.reshape(8192),capital


def solution(mesh):
    finer=Mesh(mesh.devices.reshape(4,4,8,mesh.shape["grid"]),(X,Y,ZC,G))
    in_specs=(P(None,AGENT),P(),P(),P(),P(),P(),P(),P(AGENT),P(None,AGENT),P(None,AGENT),P())
    out_specs=(P(AGENT,G),P(AGENT,G),P(AGENT),P())
    return jax.shard_map(on_device,mesh=finer,in_specs=in_specs,out_specs=out_specs,check_vma=False)
```

```python
import jax
import jax.numpy as jnp
from jax import lax
from jax.experimental import pallas as pl
from jax.experimental.pallas import tpu as pltpu
from jax.sharding import Mesh
from jax.sharding import PartitionSpec as P
MESH=pl.DeviceIdType.MESH
X,Y,ZC,G="agent_0","agent_1","agent_2","grid"
AGENT=(X,Y,ZC)
f32=jnp.float32
i32=jnp.int32
LOG2E=1.4426950408889634
KT=500.0*LOG2E
SP=40.0/15
UN=128

def hat(x,k):
    return jnp.maximum(0.0,1.0-jnp.abs(x-40.0*k/15)/SP)

def rdma(src,dst,ss,rs,**dev):
    return pltpu.make_async_remote_copy(src_ref=src,dst_ref=dst,send_sem=ss,recv_sem=rs,device_id=dev_ids(dev),device_id_type=MESH)
def dev_ids(dev):
    return {dict(x=X,y=Y,z=ZC,g=G)[k]:v for k,v in dev.items()}
def got(ref,sem):
    pltpu.make_async_copy(ref,ref,sem).wait()


CH=((0,8),(8,6),(14,2))

def life(vt_hbm, tw_hbm, hold_hbm, shock_hbm, brack_hbm, coef_ref, const_ref, int_ref, wage_ref, eff_ref, agg_ref,
         v_ref, p_ref, h_ref, cap_ref,
         vt_ref,tw_ref,hold_ref,shock_ref,brack_ref,send,mid,recv,
         pt,kpt,sc,rs,vb,pb,
         pxa,pxb,pxc,y0a,y0b,y0c,z0a,z0b,z0c,yba,ybb,ybc,lk,tt,oh,resa,resb,ri,li,own,pbk,inv,fr_s,hp,hr,pay1,in1,pay2,in2,wt,sl,sd,cl,ctot,cp,c1,c2,c3,
         sin,sa1,ra1,sa2,ra2,sx,rx,sy0,ry0,sz0,rz0,szt,rzt,sya,rya,syb,ryb,sh,rh,s1,r1,s2,r2,sc1,rc1,sc2,rc2,sc3,rc3):
    px=(pxa,pxb,pxc); y0=(y0a,y0b,y0c); z0=(z0a,z0b,z0c); yb=(yba,ybb,ybc); res=(resa,resb)
    x=lax.axis_index(X); y=lax.axis_index(Y); zc=lax.axis_index(ZC); g=lax.axis_index(G)
    inputs=[pltpu.make_async_copy(a,b,sin.at[n]) for n,(a,b) in enumerate(((vt_hbm,vt_ref),(tw_hbm,tw_ref),(hold_hbm,hold_ref),(shock_hbm,shock_ref),(brack_hbm,brack_ref)))]
    for c in inputs:
        c.start()
    bar=pltpu.get_barrier_semaphore()
    me_p=x*4+y
    me_l=zc*2+g
    def plane(d):
        o=lax.rem(me_p+d,16)
        return {X:o//4,Y:lax.rem(o,4)}
    def line(d):
        o=lax.rem(me_l+d,16)
        return {ZC:o//2,G:lax.rem(o,2)}
    def sig(d,_):
        pl.semaphore_signal(bar,inc=1,device_id=plane(d),device_id_type=MESH)
        pl.semaphore_signal(bar,inc=1,device_id=line(d),device_id_type=MESH)
        return 0
    lax.fori_loop(1,16,sig,0)

    lane8=lax.broadcasted_iota(i32,(8,128),1)
    sub8=lax.broadcasted_iota(i32,(8,128),0)
    def expect():
        inputs[0].wait(); inputs[1].wait()
        tw=tw_ref[...]
        tn=tw/jnp.sum(tw,axis=1,keepdims=True)
        blocks=[]
        for k in range(16):
            b=None
            for q in range(4):
                col=(q*4+k//4)*128
                w=vt_ref[:,col:col+128]
                d=(q*32-(k%4)*32)%128
                if d: w=pltpu.roll(w,d,1)
                b=w if b is None else jnp.where(lane8//32==q,w,b)
            blocks.append(b)
        vk=jnp.concatenate(blocks,axis=0)
        bl=lax.dot_general(vk,tn,(((1,),(1,)),((),())),precision=lax.Precision.HIGHEST,preferred_element_type=f32)
        zl=lane8//32
        def per_zone(r):
            return jnp.where(zl==0,r[0],jnp.where(zl==1,r[1],jnp.where(zl==2,r[2],r[3])))
        cf=per_zone(coef_ref); cs=per_zone(const_ref)
        masks=[(lane8//16-sub8)%8==d for d in range(8)]
        for j in range(16):
            fc=jnp.clip(cf*(40.0*j/15)+cs,0.0,40.0)
            acc=None
            for k in range(16):
                w=hat(fc,k)*bl[k*8:k*8+8,:]
                acc=w if acc is None else acc+w
            o=acc
            for d in range(1,8):
                o=jnp.where(masks[d],pltpu.roll(pltpu.roll(acc,8-d,0),16*d,1),o)
            for q in range(8):
                send[(j%4)*2+q%2,(q//2)*4+j//4]=o[q:q+1,:]
    def expect_a():
        def go(d,_):
            o=lax.rem(zc+d,8)
            rdma(send.at[o],mid.at[zc],sa1,ra1,z=o).start()
            return 0
        lax.fori_loop(1,8,go,0)
        mid[zc]=send[zc]
    def expect_b():
        got(mid.at[pl.ds(0,7)],ra1)
        def go(d,_):
            o=lax.rem(me_p+d,16)
            rdma(mid.at[:,o],recv.at[me_p],sa2,ra2,x=o//4,y=lax.rem(o,4)).start()
            return 0
        lax.fori_loop(1,16,go,0)
        recv[me_p]=mid[:,me_p]
    def expect_c():
        got(recv.at[pl.ds(0,15)],ra2)
        for q in range(16):
            rs[q*8:q*8+8,:]=jnp.concatenate([recv[q,n] for n in range(8)],axis=0)*(48.0*LOG2E)

    def pts(A,_):
        for n in range(8):
            t=A*8+n
            j=(64*A+n+8*sub8).astype(f32)
            fr=j/1023.0
            p=40.0*fr*fr
            o=pl.multiple_of(t*8,8)
            pt[pl.ds(o,8),:]=p
            kpt[pl.ds(o,8),:]=p*KT+0.1*KT
        return 0
    k=y*4+zc//2
    eh=lax.rem(zc,2)
    growth=1.0+int_ref[x,k]
    wage=wage_ref[x,k]
    def state(e,_):
        inc=wage*eff_ref[eh*16+e]
        W=[];KW=[]
        for v in range(4):
            i=(lax.broadcasted_iota(i32,(8,128),1)+(128*v+512*g)).astype(f32)
            fr=i/1023.0
            w=(40.0*fr*fr)*growth+inc
            W.append(w);KW.append(w*KT)
        def p1(c,M):
            M=list(M)
            for u in range(UN):
                off=pl.multiple_of((c*UN+u)*8,8)
                P=pt[pl.ds(off,8),:]; KP=kpt[pl.ds(off,8),:]
                Rr=rs[pl.ds(pl.multiple_of((c*(UN//8)+u//8)*8,8),8),:]
                B=jnp.take_along_axis(Rr,jnp.full((8,128),(u%8)*16+e,i32),axis=1,mode="promise_in_bounds")
                D=B-KP
                for v in range(4):
                    cl=jnp.maximum(W[v]-P,0.1)
                    S=jnp.log(cl)*(50.0*LOG2E)+jnp.minimum(KW[v]+D,B)
                    sc[pl.ds(off,8),128*v:128*v+128]=S
                    M[v]=jnp.maximum(M[v],S)
            return tuple(M)
        M=lax.fori_loop(0,128//UN,p1,tuple(jnp.full((8,128),-1e30,f32) for _ in range(4)))
        def p2(c,acc):
            acc=list(acc)
            for u in range(UN):
                off=pl.multiple_of((c*UN+u)*8,8)
                P=pt[pl.ds(off,8),:]
                for v in range(4):
                    q=jnp.exp2(sc[pl.ds(off,8),128*v:128*v+128]-M[v])
                    acc[v]=acc[v]+q
                    acc[4+v]=acc[4+v]+P*q
            return tuple(acc)
        acc=lax.fori_loop(0,128//UN,p2,tuple(jnp.zeros((8,128),f32) for _ in range(8)))
        for v in range(4):
            m=jnp.max(M[v],axis=0,keepdims=True)
            s=jnp.exp2(M[v]-m)
            tot=jnp.sum(acc[v]*s,axis=0,keepdims=True)
            q=jnp.sum(acc[4+v]*s,axis=0,keepdims=True)
            vb[e,:,128*v:128*v+128]=jnp.broadcast_to((0.02/LOG2E)*m+0.02*jnp.log(tot),(8,128))
            pb[e,:,128*v:128*v+128]=jnp.broadcast_to(q/tot,(8,128))
        return 0
    def bell(a,b):
        lax.fori_loop(a,b,state,0)
    def finish(c):
        a,n=CH[c]
        v_ref[a:a+n,:]=jnp.concatenate([vb[a+q,0:1,:] for q in range(n)],axis=0)
        p=jnp.concatenate([pb[a+q,0:1,:] for q in range(n)],axis=0)
        p_ref[a:a+n,:]=p
        px[c][x]=p

    def send_x(c):
        def go(d,_):
            rdma(px[c].at[x],px[c].at[x],sx.at[c],rx.at[c],x=lax.rem(x+d,4)).start()
            return 0
        lax.fori_loop(1,4,go,0)
    def send_y0(c,w):
        got(px[c].at[pl.ds(0,3)],rx.at[c])
        y0[c][y]=px[c][agg_ref[0]]*w
        def go(d,_):
            rdma(y0[c].at[y],y0[c].at[y],sy0.at[c],ry0.at[c],y=lax.rem(y+d,4)).start()
            return 0
        lax.fori_loop(1,4,go,0)
    def send_z0(c):
        got(y0[c].at[pl.ds(0,3)],ry0.at[c])
        b=y0[c]
        z0[c][zc]=(b[0]+b[1])+(b[2]+b[3])
        def go(d,_):
            rdma(z0[c].at[zc],z0[c].at[zc],sz0.at[c],rz0.at[c],z=lax.rem(zc+d,8)).start()
            return 0
        lax.fori_loop(1,8,go,0)
    def table0(c):
        got(z0[c].at[pl.ds(0,7)],rz0.at[c])
        a,n=CH[c]
        b=z0[c]
        for h in range(2):
            lk[h*16+a:h*16+a+n,:]=(b[h]+b[2+h])+(b[4+h]+b[6+h])
    def send_slot(t,half):
        b=yb[half]
        b[t-1,y,zc]=px[half][agg_ref[t]]
        def go(d,_):
            rdma(b.at[t-1,y,zc],b.at[t-1,y,zc],szt.at[t-1,half],rzt.at[t-1,half],z=lax.rem(zc+d,8)).start()
            return 0
        lax.fori_loop(1,8,go,0)
    up=lax.rem(y+1,4); down=lax.rem(y+3,4)
    def slot_a(t,half):
        b=yb[half]
        got(b.at[t-1,0,pl.ds(0,7)],rzt.at[t-1,half])
        for n,d in ((0,up),(1,down)):
            rdma(b.at[t-1,y],b.at[t-1,y],sya.at[t-1,half,n],rya.at[t-1,half,n],y=d).start()
    def slot_b(t,half):
        b=yb[half]
        got(b.at[t-1,0],rya.at[t-1,half,0])
        rdma(b.at[t-1,down,pl.ds(0,4)],b.at[t-1,down,pl.ds(0,4)],syb.at[t-1,half,0],ryb.at[t-1,half,0],y=up).start()
        got(b.at[t-1,0],rya.at[t-1,half,1])
        rdma(b.at[t-1,up,pl.ds(4,4)],b.at[t-1,up,pl.ds(4,4)],syb.at[t-1,half,1],ryb.at[t-1,half,1],y=down).start()
    def slot_done(t):
        for half in range(3):
            b=yb[half]
            got(b.at[t-1,0,pl.ds(0,4)],ryb.at[t-1,half,0])
            got(b.at[t-1,0,pl.ds(0,4)],ryb.at[t-1,half,1])
    def table(t,cap):
        hs=[hat(cap,q) for q in range(16)]
        for h in range(2):
            for c,(o,n) in enumerate(CH):
                for v in range(4):
                    acc=None
                    for q in range(16):
                        w=hs[q]*yb[c][t-1,q//4,2*(q%4)+h,:,128*v:128*v+128]
                        acc=w if acc is None else acc+w
                    lk[h*16+o:h*16+o+n,128*v:128*v+128]=acc

    def sum_a(t,row):
        pay1[t]=row
        in1[t,me_l]=row
        def go(d,_):
            pltpu.make_async_remote_copy(src_ref=pay1.at[t],dst_ref=in1.at[t,me_l],send_sem=s1.at[t],recv_sem=r1.at[t],device_id=line(d),device_id_type=MESH).start()
            return 0
        lax.fori_loop(1,16,go,0)
    def total(buf,t):
        rows=[buf[t,n] for n in range(16)]
        while len(rows)>1:
            rows=[rows[2*n]+rows[2*n+1] for n in range(len(rows)//2)]
        return rows[0]
    def sum_b(t):
        got(in1.at[t,pl.ds(0,15)],r1.at[t])
        row=total(in1,t)
        pay2[t]=row
        in2[t,me_p]=row
        def go(d,_):
            pltpu.make_async_remote_copy(src_ref=pay2.at[t],dst_ref=in2.at[t,me_p],send_sem=s2.at[t],recv_sem=r2.at[t],device_id=plane(d),device_id_type=MESH).start()
            return 0
        lax.fori_loop(1,16,go,0)
    def sum_c(t):
        got(in2.at[t,pl.ds(0,15)],r2.at[t])
        return total(in2,t)
    def mean_of(t,row):
        cap=jnp.sum(row)/1048576.0
        cap_ref[t]=cap
        return cap

    def index(n,_):
        cols=pl.ds(pl.multiple_of(n*1024,1024),1024)
        b=brack_ref[:,cols]; e=shock_ref[:,cols]
        edge=jnp.logical_and(b==511,g==1)
        mine=(b//512)==g
        r=((b//128)%4)*32+e
        ri[:,cols]=jnp.where(mine,r,jnp.where(edge,96+e,-1))
        li[:,cols]=jnp.where(edge,127,b%128)
        own[:,cols]=jnp.where(edge,0.0,1.0)
        fa=b.astype(f32)/1023.0; fb=(b+1).astype(f32)/1023.0
        lo=40.0*fa*fa; hi=40.0*fb*fb
        pbk[:,cols]=lo
        inv[:,cols]=1.0/(hi-lo)
        return 0
    lane=lax.broadcasted_iota(i32,(32,128),1)
    iota=lax.broadcasted_iota(i32,(128,128),0)
    def hot(t):
        def go(n,_):
            for q in range(8):
                cols=pl.ds(pl.multiple_of(n*1024+q*128,128),128)
                o=jnp.where(jnp.broadcast_to(ri[t:t+1,cols],(128,128))==iota,1.0,0.0).astype(jnp.bfloat16)
                oh[t,0:128,cols]=o
                oh[t,128:256,cols]=o
            return 0
        lax.fori_loop(0,8,go,0)
    def shares(t):
        for n in range(8):
            r8=slice(n*8,n*8+8)
            h=hold_ref[r8,:] if t==0 else hp[t-1,r8,:]+hr[t-1,r8,:]
            for q in range(8):
                cols=slice((n*8+q)*128,(n*8+q)*128+128)
                fr_s[t:t+1,cols]=jnp.clip((h[q:q+1,:]-pbk[t:t+1,cols])*inv[t:t+1,cols],0.0,1.0)
    def gather(t,between=None):
        ls=[lk[:,128*v:128*v+128] for v in range(4)]
        ro=[pltpu.roll(q,127,1) for q in ls]
        ds=[jnp.where(lane==127,ro[v+1],ro[v])-ls[v] for v in range(3)]
        first=jnp.broadcast_to(ls[0][:,0:1],(32,128))
        last=jnp.where(g==1,first,-ls[3])
        ds.append(jnp.where(lane==127,last,ro[3]-ls[3]))
        for o,q in ((0,ls),(128,ds)):
            m=jnp.concatenate(q,axis=0).T
            hi=m.astype(jnp.bfloat16)
            tt[o:o+128,0:128]=hi
            tt[o:o+128,128:256]=(m-hi.astype(f32)).astype(jnp.bfloat16)
        table_now=tt[...]
        for n in range(8):
            if n==2 and between is not None:
                between()
            rb=res[n%2]
            rb[...]=jnp.dot(table_now,oh[t,:,n*1024:n*1024+1024],preferred_element_type=f32)
            for q in range(8):
                cols=slice(n*1024+q*128,n*1024+q*128+128)
                m=jnp.broadcast_to(li[t:t+1,cols],(128,128))==iota
                sl[:,cols]=own[t:t+1,cols]*jnp.sum(jnp.where(m,rb[0:128,q*128:q*128+128],0.0),axis=0,keepdims=True)
                sd[:,cols]=jnp.sum(jnp.where(m,rb[128:256,q*128:q*128+128],0.0),axis=0,keepdims=True)
    def combine(t):
        acc=None
        for n in range(8):
            rows=[]
            for q in range(8):
                cols=slice(n*1024+q*128,n*1024+q*128+128)
                rows.append(sl[:,cols]+fr_s[t:t+1,cols]*sd[:,cols])
            hn=jnp.concatenate(rows,axis=0)
            hp[t,n*8:n*8+8,:]=hn
            acc=hn if acc is None else acc+hn
        rdma(hp.at[t],hr.at[t],sh.at[t],rh.at[t],g=1-g).start()
        return jnp.sum(acc,axis=0,keepdims=True)
    def counts(t):
        acc=None
        for n in range(8):
            for q in range(8):
                cols=slice(n*1024+q*128,n*1024+q*128+128)
                m=jnp.broadcast_to(li[t:t+1,cols],(128,128))==iota
                wt[0:128,q*128:q*128+128]=jnp.where(m,jnp.broadcast_to(own[t:t+1,cols],(128,128)),0.0).astype(jnp.bfloat16)
            d=lax.dot_general(oh[t,0:128,n*1024:n*1024+1024],wt[0:128,:],(((1,),(1,)),((),())),preferred_element_type=f32)
            acc=d if acc is None else acc+d
        cl[...]=acc
    def weights(t,between=None):
        acc=None
        for n in range(8):
            if n==4 and between is not None:
                between()
            for q in range(8):
                cols=slice(n*1024+q*128,n*1024+q*128+128)
                m=jnp.broadcast_to(li[t:t+1,cols],(128,128))==iota
                f=fr_s[t:t+1,cols]
                hi=f.astype(jnp.bfloat16).astype(f32)
                wt[0:128,q*128:q*128+128]=jnp.where(m,jnp.broadcast_to(hi,(128,128)),0.0).astype(jnp.bfloat16)
                wt[128:256,q*128:q*128+128]=jnp.where(m,jnp.broadcast_to(f-hi,(128,128)),0.0).astype(jnp.bfloat16)
            d=lax.dot_general(oh[t,0:128,n*1024:n*1024+1024],wt[...],(((1,),(1,)),((),())),preferred_element_type=f32)
            acc=d if acc is None else acc+d
        cd=acc[:,0:128]+acc[:,128:256]
        cs=[cd[32*v:32*v+32,:] for v in range(4)]
        ro=[pltpu.roll(q,1,1) for q in cs]
        for v in range(4):
            if v==3:
                inner=jnp.where(lane==127,0.0,cs[3])
                ctot_v=cl[96:128,:]-inner
                ctot_v=ctot_v-jnp.where(jnp.logical_and(lane==127,g==0),cs[3],0.0)
            else:
                ctot_v=cl[32*v:32*v+32,:]-cs[v]
            prev=ro[v-1] if v else jnp.where(g==1,ro[3],jnp.zeros_like(ro[3]))
            ctot[:,128*v:128*v+128]=ctot_v+jnp.where(lane==0,prev,ro[v])
    lane1=lax.broadcasted_iota(i32,(1,128),1)
    def moments(t,row):
        out=jnp.where(lane1==16,jnp.sum(row,axis=1,keepdims=True),0.0)
        for q in range(16):
            m=None
            for c,(o,n) in enumerate(CH):
                acc=None
                for h in range(2):
                    for v in range(4):
                        w=ctot[h*16+o:h*16+o+n,128*v:128*v+128]*yb[c][t-1,q//4,2*(q%4)+h,:,128*v:128*v+128]
                        acc=w if acc is None else acc+w
                acc=jnp.sum(acc,axis=0,keepdims=True)
                m=acc if m is None else m+acc
            m=jnp.sum(m,axis=1,keepdims=True)
            out=jnp.where(lane1==q,m,out)
        return out

    def spread_a():
        for q in range(8):
            o=(q%2)*16+(q//2)*4
            cp[q]=ctot[o:o+4,:]
        c1[zc]=cp[zc]
        def go(d,_):
            o=lax.rem(zc+d,8)
            rdma(cp.at[o],c1.at[zc],sc1,rc1,z=o).start()
            return 0
        lax.fori_loop(1,8,go,0)
    def added(b,n):
        rows=[b[q] for q in range(n)]
        while len(rows)>1:
            rows=[rows[2*q]+rows[2*q+1] for q in range(len(rows)//2)]
        return rows[0]
    def spread_b():
        got(c1.at[pl.ds(0,7)],rc1)
        c2[me_p]=added(c1,8)
        def go(d,_):
            o=lax.rem(me_p+d,16)
            rdma(c2.at[me_p],c2.at[me_p],sc2,rc2,x=o//4,y=lax.rem(o,4)).start()
            return 0
        lax.fori_loop(1,16,go,0)
    def spread_c():
        got(c2.at[pl.ds(0,15)],rc2)
        c3[zc//2]=added(c2,16)
        def go(d,_):
            rdma(c3.at[zc//2],c3.at[zc//2],sc3,rc3,z=lax.rem(zc+2*d,8)).start()
            return 0
        lax.fori_loop(1,4,go,0)
    def first_mean(w):
        got(c3.at[pl.ds(0,3)],rc3)
        acc=None
        for q in range(4):
            w4=c3[q]*p_ref[q*4:q*4+4,:]
            acc=w4 if acc is None else acc+w4
        row=jnp.sum(acc,axis=0,keepdims=True)
        row=(row[:,0:128]+row[:,128:256])+(row[:,256:384]+row[:,384:512])
        return row*(w*jnp.where(agg_ref[0]==x,1.0,0.0))

    expect()
    pl.semaphore_wait(bar,30)
    expect_a()
    for c in inputs[2:]:
        c.wait()
    h0=jnp.zeros((8,128),f32)
    for n in range(4):
        h0=h0+hold_ref[pl.ds(pl.multiple_of(g*32+n*8,8),8),:]
    sum_a(0,jnp.sum(h0,axis=0,keepdims=True))
    lax.fori_loop(0,8,index,0)
    shares(0)
    hot(0)
    lax.fori_loop(0,16,pts,0)
    expect_b()
    counts(0)
    sum_b(0)
    weights(0)
    spread_a()
    expect_c()
    bell(0,4)
    row=sum_c(0)
    cap=mean_of(0,row)
    kf=k.astype(f32)
    w0=jnp.maximum(0.0,1.0-jnp.abs(cap-40.0*kf/15)/SP)
    spread_b()
    bell(4,8)
    finish(0)
    send_x(0)
    spread_c()
    bell(8,11)
    send_y0(0,w0)
    send_slot(1,0)
    bell(11,14)
    finish(1)
    send_x(1)
    send_z0(0)
    bell(14,16)
    finish(2)
    send_x(2)
    sum_a(1,first_mean(w0))
    send_y0(1,w0)
    send_slot(1,1)
    hot(1)
    send_y0(2,w0)
    send_slot(1,2)
    send_z0(1)
    slot_a(1,0)
    send_z0(2)
    send_slot(2,0)
    sum_b(1)
    hot(2)
    send_slot(2,1)
    send_slot(2,2)
    slot_a(1,1)
    slot_a(1,2)
    slot_b(1,0)
    table0(0)
    table0(1)
    table0(2)
    def later():
        slot_b(1,1)
        slot_b(1,2)
    gather(0,later)
    combine(0)
    for n in range(3):
        send_slot(3,n)
    cap=mean_of(1,sum_c(1))
    slot_a(2,0)
    slot_done(1)
    slot_a(2,1)
    slot_a(2,2)
    table(1,cap)
    gather(1)
    got(hr.at[0],rh.at[0])
    shares(1)
    row=combine(1)
    counts(2)
    slot_b(2,0)
    got(hr.at[1],rh.at[1])
    shares(2)
    def later2():
        slot_b(2,1)
        slot_b(2,2)
        for n in range(3):
            slot_a(3,n)
    weights(2,later2)
    slot_done(2)
    sum_a(2,moments(2,row))
    hot(3)
    sum_b(2)
    for n in range(3):
        slot_b(3,n)
    row=sum_c(2)
    cap=jnp.sum(jnp.where(lane1==16,row,0.0))/1048576.0
    cap_ref[2]=cap
    table(2,cap)
    qs=lane1.astype(f32)*40.0/15
    cap3=jnp.sum(jnp.where(lane1<16,jnp.maximum(0.0,1.0-jnp.abs(cap-qs)/SP)*row,0.0))/1048576.0
    cap_ref[3]=cap3
    gather(2)
    combine(2)
    slot_done(3)
    table(3,cap3)
    gather(3)
    got(hr.at[2],rh.at[2])
    shares(3)
    combine(3)
    got(hr.at[3],rh.at[3])
    h_ref[...]=hp[3]+hr[3]
    got(mid.at[pl.ds(0,7)],sa1)
    got(recv.at[pl.ds(0,15)],sa2)
    got(c1.at[pl.ds(0,7)],sc1)
    got(c2.at[pl.ds(0,15)],sc2)
    got(c3.at[pl.ds(0,3)],sc3)
    for c in range(3):
        got(px[c].at[pl.ds(0,3)],sx.at[c])
        got(y0[c].at[pl.ds(0,3)],sy0.at[c])
        got(z0[c].at[pl.ds(0,7)],sz0.at[c])
    for t in range(3):
        for half in range(3):
            b=yb[half]
            got(b.at[t,0,pl.ds(0,7)],szt.at[t,half])
            for n in range(2):
                got(b.at[t,0],sya.at[t,half,n])
                got(b.at[t,0,pl.ds(0,4)],syb.at[t,half,n])
    for t in range(4):
        got(hp.at[t],sh.at[t])
    for t in range(3):
        got(in1.at[t,pl.ds(0,15)],s1.at[t])
        got(in2.at[t,pl.ds(0,15)],s2.at[t])

def life_call(vt,tw,hold,shock,brack,coef,const,interest,wage,eff,agg):
    vm=pl.BlockSpec(memory_space=pltpu.VMEM); sm=pl.BlockSpec(memory_space=pltpu.SMEM); hb=pl.BlockSpec(memory_space=pltpu.HBM)
    V=lambda *s: pltpu.VMEM(s,f32)
    B=lambda *s: pltpu.VMEM(s,jnp.bfloat16)
    I=lambda *s: pltpu.VMEM(s,i32)
    S=lambda *s: pltpu.SemaphoreType.DMA(s)
    one=pltpu.SemaphoreType.DMA
    return pl.pallas_call(life,
        out_shape=[jax.ShapeDtypeStruct((16,512),f32),jax.ShapeDtypeStruct((16,512),f32),jax.ShapeDtypeStruct((64,128),f32),jax.ShapeDtypeStruct((4,),f32)],
        in_specs=[hb]*5+[sm]*6,out_specs=[vm,vm,vm,sm],
        scratch_shapes=[V(8,2048),V(128,128),V(64,128),I(4,8192),I(4,8192),V(8,16,1,128),V(8,16,1,128),V(16,8,1,128),
            V(1024,128),V(1024,128),V(1024,512),V(128,128),V(16,8,512),V(16,8,512),
            V(4,8,512),V(4,6,512),V(4,2,512),V(4,8,512),V(4,6,512),V(4,2,512),V(8,8,512),V(8,6,512),V(8,2,512),
            V(3,4,8,8,512),V(3,4,8,6,512),V(3,4,8,2,512),V(32,512),B(256,256),B(4,256,8192),V(256,1024),V(256,1024),
            I(4,8192),I(4,8192),V(4,8192),V(4,8192),V(4,8192),V(4,8192),V(4,64,128),V(4,64,128),V(3,1,128),V(3,16,1,128),V(3,1,128),V(3,16,1,128),
            B(256,1024),V(1,8192),V(1,8192),V(128,128),V(32,512),V(8,4,512),V(8,4,512),V(16,4,512),V(4,4,512),
            S(5),one,one,one,one,S(3),S(3),S(3),S(3),S(3),S(3),S(3,3),S(3,3),S(3,3,2),S(3,3,2),S(3,3,2),S(3,3,2),S(4),S(4),S(3),S(3),S(3),S(3),one,one,one,one,one,one],
        compiler_params=pltpu.CompilerParams(collective_id=1,has_side_effects=True,vmem_limit_bytes=60*1024*1024),name="life")(vt,tw,hold,shock,brack,coef,const,interest,wage,eff,agg)

def put_out(v,p,h,c,vo,po,ho,co,sem):
    copies=[pltpu.make_async_copy(a,b,sem.at[n]) for n,(a,b) in enumerate(((v,vo),(p,po),(h,ho)))]
    for q in copies:
        q.start()
    for n in range(4):
        co[n]=c[n]
    for q in copies:
        q.wait()

def put_out_call(v,p,h,c):
    vm=pl.BlockSpec(memory_space=pltpu.VMEM); sm=pl.BlockSpec(memory_space=pltpu.SMEM); hb=pl.BlockSpec(memory_space=pltpu.HBM)
    return pl.pallas_call(put_out,out_shape=[jax.ShapeDtypeStruct(a.shape,f32) for a in (v,p,h,c)],in_specs=[hb,hb,hb,sm],out_specs=[hb,hb,hb,sm],
        scratch_shapes=[pltpu.SemaphoreType.DMA((3,))],name="put_out")(v,p,h,c)


def on_device(value_prior,trans_weight,coefficient,constant,interest,wage_level,efficiency,holdings,shocks,brackets,aggregate):
    values_now,policy,final,capital=life_call(value_prior.T,trans_weight,holdings.reshape(64,128),shocks,brackets,coefficient,constant,interest,wage_level,efficiency,aggregate)
    values_now,policy,final,capital=put_out_call(values_now,policy,final,capital)
    return values_now,policy,final.reshape(8192),capital


def solution(mesh):
    finer=Mesh(mesh.devices.reshape(4,4,8,mesh.shape["grid"]),(X,Y,ZC,G))
    in_specs=(P(None,AGENT),P(),P(),P(),P(),P(),P(),P(AGENT),P(None,AGENT),P(None,AGENT),P())
    out_specs=(P(AGENT,G),P(AGENT,G),P(AGENT),P())
    return jax.shard_map(on_device,mesh=finer,in_specs=in_specs,out_specs=out_specs,check_vma=False)
```

```python
import jax
import jax.numpy as jnp
from jax import lax
from jax.experimental import pallas as pl
from jax.experimental.pallas import tpu as pltpu
from jax.sharding import Mesh
from jax.sharding import PartitionSpec as P
MESH=pl.DeviceIdType.MESH
X,Y,ZC,G="agent_0","agent_1","agent_2","grid"
AGENT=(X,Y,ZC)
f32=jnp.float32
i32=jnp.int32
LOG2E=1.4426950408889634
KT=500.0*LOG2E
SP=40.0/15
UN=128

def hat(x,k):
    return jnp.maximum(0.0,1.0-jnp.abs(x-40.0*k/15)/SP)

def rdma(src,dst,ss,rs,**dev):
    return pltpu.make_async_remote_copy(src_ref=src,dst_ref=dst,send_sem=ss,recv_sem=rs,device_id=dev_ids(dev),device_id_type=MESH)
def dev_ids(dev):
    return {dict(x=X,y=Y,z=ZC,g=G)[k]:v for k,v in dev.items()}
def got(ref,sem):
    pltpu.make_async_copy(ref,ref,sem).wait()


CH=((0,8),(8,6),(14,2))

def life(vt_hbm, tw_hbm, hold_hbm, shock_hbm, brack_hbm, coef_ref, const_ref, int_ref, wage_ref, eff_ref, agg_ref,
         v_ref, p_ref, h_ref, cap_ref,
         vt_ref,tw_ref,hold_ref,shock_ref,brack_ref,send,mid,recv,
         pt,kpt,sc,rs,vb,pb,
         pxa,pxb,pxc,y0a,y0b,y0c,z0a,z0b,z0c,yba,ybb,ybc,lk,tt,oh,resa,resb,ri,li,own,pbk,inv,fr_s,hp,hr,pay1,in1,pay2,in2,wt,sl,sd,cl,ctot,cp,c1,c2,c3,
         sin,sa1,ra1,sa2,ra2,sx,rx,sy0,ry0,sz0,rz0,szt,rzt,sya,rya,syb,ryb,sh,rh,s1,r1,s2,r2,sc1,rc1,sc2,rc2,sc3,rc3):
    px=(pxa,pxb,pxc); y0=(y0a,y0b,y0c); z0=(z0a,z0b,z0c); yb=(yba,ybb,ybc); res=(resa,resb)
    x=lax.axis_index(X); y=lax.axis_index(Y); zc=lax.axis_index(ZC); g=lax.axis_index(G)
    inputs=[pltpu.make_async_copy(a,b,sin.at[n]) for n,(a,b) in enumerate(((vt_hbm,vt_ref),(tw_hbm,tw_ref),(hold_hbm,hold_ref),(shock_hbm,shock_ref),(brack_hbm,brack_ref)))]
    for c in inputs:
        c.start()
    bar=pltpu.get_barrier_semaphore()
    me_p=x*4+y
    me_l=zc*2+g
    def plane(d):
        o=lax.rem(me_p+d,16)
        return {X:o//4,Y:lax.rem(o,4)}
    def line(d):
        o=lax.rem(me_l+d,16)
        return {ZC:o//2,G:lax.rem(o,2)}
    def sig(d,_):
        pl.semaphore_signal(bar,inc=1,device_id=plane(d),device_id_type=MESH)
        pl.semaphore_signal(bar,inc=1,device_id=line(d),device_id_type=MESH)
        return 0
    lax.fori_loop(1,16,sig,0)

    lane8=lax.broadcasted_iota(i32,(8,128),1)
    sub8=lax.broadcasted_iota(i32,(8,128),0)
    def expect():
        inputs[0].wait(); inputs[1].wait()
        tw=tw_ref[...]
        tn=tw/jnp.sum(tw,axis=1,keepdims=True)
        blocks=[]
        for k in range(16):
            b=None
            for q in range(4):
                col=(q*4+k//4)*128
                w=vt_ref[:,col:col+128]
                d=(q*32-(k%4)*32)%128
                if d: w=pltpu.roll(w,d,1)
                b=w if b is None else jnp.where(lane8//32==q,w,b)
            blocks.append(b)
        vk=jnp.concatenate(blocks,axis=0)
        bl=lax.dot_general(vk,tn,(((1,),(1,)),((),())),precision=lax.Precision.HIGHEST,preferred_element_type=f32)
        zl=lane8//32
        def per_zone(r):
            return jnp.where(zl==0,r[0],jnp.where(zl==1,r[1],jnp.where(zl==2,r[2],r[3])))
        cf=per_zone(coef_ref); cs=per_zone(const_ref)
        masks=[(lane8//16-sub8)%8==d for d in range(8)]
        for j in range(16):
            fc=jnp.clip(cf*(40.0*j/15)+cs,0.0,40.0)
            acc=None
            for k in range(16):
                w=hat(fc,k)*bl[k*8:k*8+8,:]
                acc=w if acc is None else acc+w
            o=acc
            for d in range(1,8):
                o=jnp.where(masks[d],pltpu.roll(pltpu.roll(acc,8-d,0),16*d,1),o)
            for q in range(8):
                send[(j%4)*2+q%2,(q//2)*4+j//4]=o[q:q+1,:]
    def expect_a():
        def go(d,_):
            o=lax.rem(zc+d,8)
            rdma(send.at[o],mid.at[zc],sa1,ra1,z=o).start()
            return 0
        lax.fori_loop(1,8,go,0)
        mid[zc]=send[zc]
    def expect_b():
        got(mid.at[pl.ds(0,7)],ra1)
        def go(d,_):
            o=lax.rem(me_p+d,16)
            rdma(mid.at[:,o],recv.at[me_p],sa2,ra2,x=o//4,y=lax.rem(o,4)).start()
            return 0
        lax.fori_loop(1,16,go,0)
        recv[me_p]=mid[:,me_p]
    def expect_c():
        got(recv.at[pl.ds(0,15)],ra2)
        for q in range(16):
            rs[q*8:q*8+8,:]=jnp.concatenate([recv[q,n] for n in range(8)],axis=0)*(48.0*LOG2E)

    def pts(A,_):
        for n in range(8):
            t=A*8+n
            j=(64*A+n+8*sub8).astype(f32)
            fr=j/1023.0
            p=40.0*fr*fr
            o=pl.multiple_of(t*8,8)
            pt[pl.ds(o,8),:]=p
            kpt[pl.ds(o,8),:]=p*KT+0.1*KT
        return 0
    k=y*4+zc//2
    eh=lax.rem(zc,2)
    growth=1.0+int_ref[x,k]
    wage=wage_ref[x,k]
    def state(e,_):
        inc=wage*eff_ref[eh*16+e]
        W=[];KW=[]
        for v in range(4):
            i=(lax.broadcasted_iota(i32,(8,128),1)+(128*v+512*g)).astype(f32)
            fr=i/1023.0
            w=(40.0*fr*fr)*growth+inc
            W.append(w);KW.append(w*KT)
        def p1(c,M):
            M=list(M)
            for u in range(UN):
                off=pl.multiple_of((c*UN+u)*8,8)
                P=pt[pl.ds(off,8),:]; KP=kpt[pl.ds(off,8),:]
                Rr=rs[pl.ds(pl.multiple_of((c*(UN//8)+u//8)*8,8),8),:]
                B=jnp.take_along_axis(Rr,jnp.full((8,128),(u%8)*16+e,i32),axis=1,mode="promise_in_bounds")
                D=B-KP
                for v in range(4):
                    cl=jnp.maximum(W[v]-P,0.1)
                    S=lax.log2(cl)*50.0+jnp.minimum(KW[v]+D,B)
                    sc[pl.ds(off,8),128*v:128*v+128]=S
                    M[v]=jnp.maximum(M[v],S)
            return tuple(M)
        M=lax.fori_loop(0,128//UN,p1,tuple(jnp.full((8,128),-1e30,f32) for _ in range(4)))
        def p2(c,acc):
            acc=list(acc)
            for u in range(UN):
                off=pl.multiple_of((c*UN+u)*8,8)
                P=pt[pl.ds(off,8),:]
                for v in range(4):
                    q=jnp.exp2(sc[pl.ds(off,8),128*v:128*v+128]-M[v])
                    acc[v]=acc[v]+q
                    acc[4+v]=acc[4+v]+P*q
            return tuple(acc)
        acc=lax.fori_loop(0,128//UN,p2,tuple(jnp.zeros((8,128),f32) for _ in range(8)))
        for v in range(4):
            m=jnp.max(M[v],axis=0,keepdims=True)
            s=jnp.exp2(M[v]-m)
            tot=jnp.sum(acc[v]*s,axis=0,keepdims=True)
            q=jnp.sum(acc[4+v]*s,axis=0,keepdims=True)
            vb[e,:,128*v:128*v+128]=jnp.broadcast_to((0.02/LOG2E)*m+0.02*jnp.log(tot),(8,128))
            pb[e,:,128*v:128*v+128]=jnp.broadcast_to(q/tot,(8,128))
        return 0
    def bell(a,b):
        lax.fori_loop(a,b,state,0)
    def finish(c):
        a,n=CH[c]
        v_ref[a:a+n,:]=jnp.concatenate([vb[a+q,0:1,:] for q in range(n)],axis=0)
        p=jnp.concatenate([pb[a+q,0:1,:] for q in range(n)],axis=0)
        p_ref[a:a+n,:]=p
        px[c][x]=p

    def send_x(c):
        def go(d,_):
            rdma(px[c].at[x],px[c].at[x],sx.at[c],rx.at[c],x=lax.rem(x+d,4)).start()
            return 0
        lax.fori_loop(1,4,go,0)
    def send_y0(c,w):
        got(px[c].at[pl.ds(0,3)],rx.at[c])
        y0[c][y]=px[c][agg_ref[0]]*w
        def go(d,_):
            rdma(y0[c].at[y],y0[c].at[y],sy0.at[c],ry0.at[c],y=lax.rem(y+d,4)).start()
            return 0
        lax.fori_loop(1,4,go,0)
    def send_z0(c):
        got(y0[c].at[pl.ds(0,3)],ry0.at[c])
        b=y0[c]
        z0[c][zc]=(b[0]+b[1])+(b[2]+b[3])
        def go(d,_):
            rdma(z0[c].at[zc],z0[c].at[zc],sz0.at[c],rz0.at[c],z=lax.rem(zc+d,8)).start()
            return 0
        lax.fori_loop(1,8,go,0)
    def table0(c):
        got(z0[c].at[pl.ds(0,7)],rz0.at[c])
        a,n=CH[c]
        b=z0[c]
        for h in range(2):
            lk[h*16+a:h*16+a+n,:]=(b[h]+b[2+h])+(b[4+h]+b[6+h])
    def send_slot(t,half):
        b=yb[half]
        b[t-1,y,zc]=px[half][agg_ref[t]]
        def go(d,_):
            rdma(b.at[t-1,y,zc],b.at[t-1,y,zc],szt.at[t-1,half],rzt.at[t-1,half],z=lax.rem(zc+d,8)).start()
            return 0
        lax.fori_loop(1,8,go,0)
    up=lax.rem(y+1,4); down=lax.rem(y+3,4)
    def slot_a(t,half):
        b=yb[half]
        got(b.at[t-1,0,pl.ds(0,7)],rzt.at[t-1,half])
        for n,d in ((0,up),(1,down)):
            rdma(b.at[t-1,y],b.at[t-1,y],sya.at[t-1,half,n],rya.at[t-1,half,n],y=d).start()
    def slot_b(t,half):
        b=yb[half]
        got(b.at[t-1,0],rya.at[t-1,half,0])
        rdma(b.at[t-1,down,pl.ds(0,4)],b.at[t-1,down,pl.ds(0,4)],syb.at[t-1,half,0],ryb.at[t-1,half,0],y=up).start()
        got(b.at[t-1,0],rya.at[t-1,half,1])
        rdma(b.at[t-1,up,pl.ds(4,4)],b.at[t-1,up,pl.ds(4,4)],syb.at[t-1,half,1],ryb.at[t-1,half,1],y=down).start()
    def slot_done(t):
        for half in range(3):
            b=yb[half]
            got(b.at[t-1,0,pl.ds(0,4)],ryb.at[t-1,half,0])
            got(b.at[t-1,0,pl.ds(0,4)],ryb.at[t-1,half,1])
    def table(t,cap):
        hs=[hat(cap,q) for q in range(16)]
        for h in range(2):
            for c,(o,n) in enumerate(CH):
                for v in range(4):
                    acc=None
                    for q in range(16):
                        w=hs[q]*yb[c][t-1,q//4,2*(q%4)+h,:,128*v:128*v+128]
                        acc=w if acc is None else acc+w
                    lk[h*16+o:h*16+o+n,128*v:128*v+128]=acc

    def sum_a(t,row):
        pay1[t]=row
        in1[t,me_l]=row
        def go(d,_):
            pltpu.make_async_remote_copy(src_ref=pay1.at[t],dst_ref=in1.at[t,me_l],send_sem=s1.at[t],recv_sem=r1.at[t],device_id=line(d),device_id_type=MESH).start()
            return 0
        lax.fori_loop(1,16,go,0)
    def total(buf,t):
        rows=[buf[t,n] for n in range(16)]
        while len(rows)>1:
            rows=[rows[2*n]+rows[2*n+1] for n in range(len(rows)//2)]
        return rows[0]
    def sum_b(t):
        got(in1.at[t,pl.ds(0,15)],r1.at[t])
        row=total(in1,t)
        pay2[t]=row
        in2[t,me_p]=row
        def go(d,_):
            pltpu.make_async_remote_copy(src_ref=pay2.at[t],dst_ref=in2.at[t,me_p],send_sem=s2.at[t],recv_sem=r2.at[t],device_id=plane(d),device_id_type=MESH).start()
            return 0
        lax.fori_loop(1,16,go,0)
    def sum_c(t):
        got(in2.at[t,pl.ds(0,15)],r2.at[t])
        return total(in2,t)
    def mean_of(t,row):
        cap=jnp.sum(row)/1048576.0
        cap_ref[t]=cap
        return cap

    def index(n,_):
        cols=pl.ds(pl.multiple_of(n*1024,1024),1024)
        b=brack_ref[:,cols]; e=shock_ref[:,cols]
        edge=jnp.logical_and(b==511,g==1)
        mine=(b//512)==g
        r=((b//128)%4)*32+e
        ri[:,cols]=jnp.where(mine,r,jnp.where(edge,96+e,-1))
        li[:,cols]=jnp.where(edge,127,b%128)
        own[:,cols]=jnp.where(edge,0.0,1.0)
        fa=b.astype(f32)/1023.0; fb=(b+1).astype(f32)/1023.0
        lo=40.0*fa*fa; hi=40.0*fb*fb
        pbk[:,cols]=lo
        inv[:,cols]=1.0/(hi-lo)
        return 0
    lane=lax.broadcasted_iota(i32,(32,128),1)
    iota=lax.broadcasted_iota(i32,(128,128),0)
    def hot(t):
        def go(n,_):
            for q in range(8):
                cols=pl.ds(pl.multiple_of(n*1024+q*128,128),128)
                o=jnp.where(jnp.broadcast_to(ri[t:t+1,cols],(128,128))==iota,1.0,0.0).astype(jnp.bfloat16)
                oh[t,0:128,cols]=o
                oh[t,128:256,cols]=o
            return 0
        lax.fori_loop(0,8,go,0)
    def shares(t):
        for n in range(8):
            r8=slice(n*8,n*8+8)
            h=hold_ref[r8,:] if t==0 else hp[t-1,r8,:]+hr[t-1,r8,:]
            for q in range(8):
                cols=slice((n*8+q)*128,(n*8+q)*128+128)
                fr_s[t:t+1,cols]=jnp.clip((h[q:q+1,:]-pbk[t:t+1,cols])*inv[t:t+1,cols],0.0,1.0)
    def gather(t,between=None):
        ls=[lk[:,128*v:128*v+128] for v in range(4)]
        ro=[pltpu.roll(q,127,1) for q in ls]
        ds=[jnp.where(lane==127,ro[v+1],ro[v])-ls[v] for v in range(3)]
        first=jnp.broadcast_to(ls[0][:,0:1],(32,128))
        last=jnp.where(g==1,first,-ls[3])
        ds.append(jnp.where(lane==127,last,ro[3]-ls[3]))
        for o,q in ((0,ls),(128,ds)):
            m=jnp.concatenate(q,axis=0).T
            hi=m.astype(jnp.bfloat16)
            tt[o:o+128,0:128]=hi
            tt[o:o+128,128:256]=(m-hi.astype(f32)).astype(jnp.bfloat16)
        table_now=tt[...]
        for n in range(8):
            if n==3 and between is not None:
                between()
            rb=res[n%2]
            rb[...]=jnp.dot(table_now,oh[t,:,n*1024:n*1024+1024],preferred_element_type=f32)
            for q in range(8):
                cols=slice(n*1024+q*128,n*1024+q*128+128)
                m=jnp.broadcast_to(li[t:t+1,cols],(128,128))==iota
                sl[:,cols]=own[t:t+1,cols]*jnp.sum(jnp.where(m,rb[0:128,q*128:q*128+128],0.0),axis=0,keepdims=True)
                sd[:,cols]=jnp.sum(jnp.where(m,rb[128:256,q*128:q*128+128],0.0),axis=0,keepdims=True)
    def combine(t):
        acc=None
        for n in range(8):
            rows=[]
            for q in range(8):
                cols=slice(n*1024+q*128,n*1024+q*128+128)
                rows.append(sl[:,cols]+fr_s[t:t+1,cols]*sd[:,cols])
            hn=jnp.concatenate(rows,axis=0)
            hp[t,n*8:n*8+8,:]=hn
            acc=hn if acc is None else acc+hn
        rdma(hp.at[t],hr.at[t],sh.at[t],rh.at[t],g=1-g).start()
        return jnp.sum(acc,axis=0,keepdims=True)
    def counts(t):
        acc=None
        for n in range(8):
            for q in range(8):
                cols=slice(n*1024+q*128,n*1024+q*128+128)
                m=jnp.broadcast_to(li[t:t+1,cols],(128,128))==iota
                wt[0:128,q*128:q*128+128]=jnp.where(m,jnp.broadcast_to(own[t:t+1,cols],(128,128)),0.0).astype(jnp.bfloat16)
            d=lax.dot_general(oh[t,0:128,n*1024:n*1024+1024],wt[0:128,:],(((1,),(1,)),((),())),preferred_element_type=f32)
            acc=d if acc is None else acc+d
        cl[...]=acc
    def weights(t,between=None):
        acc=None
        for n in range(8):
            if n==3 and between is not None:
                between()
            for q in range(8):
                cols=slice(n*1024+q*128,n*1024+q*128+128)
                m=jnp.broadcast_to(li[t:t+1,cols],(128,128))==iota
                f=fr_s[t:t+1,cols]
                hi=f.astype(jnp.bfloat16).astype(f32)
                wt[0:128,q*128:q*128+128]=jnp.where(m,jnp.broadcast_to(hi,(128,128)),0.0).astype(jnp.bfloat16)
                wt[128:256,q*128:q*128+128]=jnp.where(m,jnp.broadcast_to(f-hi,(128,128)),0.0).astype(jnp.bfloat16)
            d=lax.dot_general(oh[t,0:128,n*1024:n*1024+1024],wt[...],(((1,),(1,)),((),())),preferred_element_type=f32)
            acc=d if acc is None else acc+d
        cd=acc[:,0:128]+acc[:,128:256]
        cs=[cd[32*v:32*v+32,:] for v in range(4)]
        ro=[pltpu.roll(q,1,1) for q in cs]
        for v in range(4):
            if v==3:
                inner=jnp.where(lane==127,0.0,cs[3])
                ctot_v=cl[96:128,:]-inner
                ctot_v=ctot_v-jnp.where(jnp.logical_and(lane==127,g==0),cs[3],0.0)
            else:
                ctot_v=cl[32*v:32*v+32,:]-cs[v]
            prev=ro[v-1] if v else jnp.where(g==1,ro[3],jnp.zeros_like(ro[3]))
            ctot[:,128*v:128*v+128]=ctot_v+jnp.where(lane==0,prev,ro[v])
    lane1=lax.broadcasted_iota(i32,(1,128),1)
    def moments(t,row):
        out=jnp.where(lane1==16,jnp.sum(row,axis=1,keepdims=True),0.0)
        for q in range(16):
            m=None
            for c,(o,n) in enumerate(CH):
                acc=None
                for h in range(2):
                    for v in range(4):
                        w=ctot[h*16+o:h*16+o+n,128*v:128*v+128]*yb[c][t-1,q//4,2*(q%4)+h,:,128*v:128*v+128]
                        acc=w if acc is None else acc+w
                acc=jnp.sum(acc,axis=0,keepdims=True)
                m=acc if m is None else m+acc
            m=jnp.sum(m,axis=1,keepdims=True)
            out=jnp.where(lane1==q,m,out)
        return out

    def spread_a():
        for q in range(8):
            o=(q%2)*16+(q//2)*4
            cp[q]=ctot[o:o+4,:]
        c1[zc]=cp[zc]
        def go(d,_):
            o=lax.rem(zc+d,8)
            rdma(cp.at[o],c1.at[zc],sc1,rc1,z=o).start()
            return 0
        lax.fori_loop(1,8,go,0)
    def added(b,n):
        rows=[b[q] for q in range(n)]
        while len(rows)>1:
            rows=[rows[2*q]+rows[2*q+1] for q in range(len(rows)//2)]
        return rows[0]
    def spread_b():
        got(c1.at[pl.ds(0,7)],rc1)
        c2[me_p]=added(c1,8)
        def go(d,_):
            o=lax.rem(me_p+d,16)
            rdma(c2.at[me_p],c2.at[me_p],sc2,rc2,x=o//4,y=lax.rem(o,4)).start()
            return 0
        lax.fori_loop(1,16,go,0)
    def spread_c():
        got(c2.at[pl.ds(0,15)],rc2)
        c3[zc//2]=added(c2,16)
        def go(d,_):
            rdma(c3.at[zc//2],c3.at[zc//2],sc3,rc3,z=lax.rem(zc+2*d,8)).start()
            return 0
        lax.fori_loop(1,4,go,0)
    def first_mean(w):
        got(c3.at[pl.ds(0,3)],rc3)
        acc=None
        for q in range(4):
            w4=c3[q]*p_ref[q*4:q*4+4,:]
            acc=w4 if acc is None else acc+w4
        row=jnp.sum(acc,axis=0,keepdims=True)
        row=(row[:,0:128]+row[:,128:256])+(row[:,256:384]+row[:,384:512])
        return row*(w*jnp.where(agg_ref[0]==x,1.0,0.0))

    expect()
    pl.semaphore_wait(bar,30)
    expect_a()
    for c in inputs[2:]:
        c.wait()
    h0=jnp.zeros((8,128),f32)
    for n in range(4):
        h0=h0+hold_ref[pl.ds(pl.multiple_of(g*32+n*8,8),8),:]
    sum_a(0,jnp.sum(h0,axis=0,keepdims=True))
    lax.fori_loop(0,8,index,0)
    shares(0)
    hot(0)
    lax.fori_loop(0,16,pts,0)
    expect_b()
    counts(0)
    sum_b(0)
    weights(0)
    spread_a()
    expect_c()
    bell(0,4)
    row=sum_c(0)
    cap=mean_of(0,row)
    kf=k.astype(f32)
    w0=jnp.maximum(0.0,1.0-jnp.abs(cap-40.0*kf/15)/SP)
    spread_b()
    bell(4,8)
    finish(0)
    send_x(0)
    spread_c()
    bell(8,11)
    send_y0(0,w0)
    send_slot(1,0)
    send_slot(2,0)
    bell(11,14)
    finish(1)
    send_x(1)
    send_z0(0)
    bell(14,16)
    finish(2)
    send_x(2)
    sum_a(1,first_mean(w0))
    send_y0(1,w0)
    send_slot(1,1)
    hot(1)
    send_y0(2,w0)
    send_slot(1,2)
    send_z0(1)
    slot_a(1,0)
    send_z0(2)
    sum_b(1)
    send_slot(2,1)
    send_slot(2,2)
    for n in range(3):
        send_slot(3,n)
    slot_a(2,0)
    hot(2)
    slot_a(1,1)
    slot_a(1,2)
    slot_b(1,0)
    table0(0)
    table0(1)
    table0(2)
    gather(0)
    combine(0)
    counts(2)
    slot_b(1,1)
    slot_b(1,2)
    slot_a(2,1)
    slot_a(2,2)
    slot_b(2,0)
    cap=mean_of(1,sum_c(1))
    slot_done(1)
    table(1,cap)
    gather(1)
    got(hr.at[0],rh.at[0])
    shares(1)
    row=combine(1)
    got(hr.at[1],rh.at[1])
    shares(2)
    slot_b(2,1)
    slot_b(2,2)
    def later2():
        for n in range(3):
            slot_a(3,n)
    weights(2,later2)
    slot_done(2)
    sum_a(2,moments(2,row))
    hot(3)
    sum_b(2)
    for n in range(3):
        slot_b(3,n)
    row=sum_c(2)
    cap=jnp.sum(jnp.where(lane1==16,row,0.0))/1048576.0
    cap_ref[2]=cap
    table(2,cap)
    qs=lane1.astype(f32)*40.0/15
    cap3=jnp.sum(jnp.where(lane1<16,jnp.maximum(0.0,1.0-jnp.abs(cap-qs)/SP)*row,0.0))/1048576.0
    cap_ref[3]=cap3
    gather(2)
    combine(2)
    slot_done(3)
    table(3,cap3)
    gather(3)
    got(hr.at[2],rh.at[2])
    shares(3)
    combine(3)
    got(mid.at[pl.ds(0,7)],sa1)
    got(recv.at[pl.ds(0,15)],sa2)
    got(c1.at[pl.ds(0,7)],sc1)
    got(c2.at[pl.ds(0,15)],sc2)
    got(c3.at[pl.ds(0,3)],sc3)
    for c in range(3):
        got(px[c].at[pl.ds(0,3)],sx.at[c])
        got(y0[c].at[pl.ds(0,3)],sy0.at[c])
        got(z0[c].at[pl.ds(0,7)],sz0.at[c])
    for t in range(3):
        for half in range(3):
            b=yb[half]
            got(b.at[t,0,pl.ds(0,7)],szt.at[t,half])
            for n in range(2):
                got(b.at[t,0],sya.at[t,half,n])
                got(b.at[t,0,pl.ds(0,4)],syb.at[t,half,n])
    for t in range(4):
        got(hp.at[t],sh.at[t])
    for t in range(3):
        got(in1.at[t,pl.ds(0,15)],s1.at[t])
        got(in2.at[t,pl.ds(0,15)],s2.at[t])
    got(hr.at[3],rh.at[3])
    h_ref[...]=hp[3]+hr[3]

def life_call(vt,tw,hold,shock,brack,coef,const,interest,wage,eff,agg):
    vm=pl.BlockSpec(memory_space=pltpu.VMEM); sm=pl.BlockSpec(memory_space=pltpu.SMEM); hb=pl.BlockSpec(memory_space=pltpu.HBM)
    V=lambda *s: pltpu.VMEM(s,f32)
    B=lambda *s: pltpu.VMEM(s,jnp.bfloat16)
    I=lambda *s: pltpu.VMEM(s,i32)
    S=lambda *s: pltpu.SemaphoreType.DMA(s)
    one=pltpu.SemaphoreType.DMA
    return pl.pallas_call(life,
        out_shape=[jax.ShapeDtypeStruct((16,512),f32),jax.ShapeDtypeStruct((16,512),f32),jax.ShapeDtypeStruct((64,128),f32),jax.ShapeDtypeStruct((4,),f32)],
        in_specs=[hb]*5+[sm]*6,out_specs=[vm,vm,vm,sm],
        scratch_shapes=[V(8,2048),V(128,128),V(64,128),I(4,8192),I(4,8192),V(8,16,1,128),V(8,16,1,128),V(16,8,1,128),
            V(1024,128),V(1024,128),V(1024,512),V(128,128),V(16,8,512),V(16,8,512),
            V(4,8,512),V(4,6,512),V(4,2,512),V(4,8,512),V(4,6,512),V(4,2,512),V(8,8,512),V(8,6,512),V(8,2,512),
            V(3,4,8,8,512),V(3,4,8,6,512),V(3,4,8,2,512),V(32,512),B(256,256),B(4,256,8192),V(256,1024),V(256,1024),
            I(4,8192),I(4,8192),V(4,8192),V(4,8192),V(4,8192),V(4,8192),V(4,64,128),V(4,64,128),V(3,1,128),V(3,16,1,128),V(3,1,128),V(3,16,1,128),
            B(256,1024),V(1,8192),V(1,8192),V(128,128),V(32,512),V(8,4,512),V(8,4,512),V(16,4,512),V(4,4,512),
            S(5),one,one,one,one,S(3),S(3),S(3),S(3),S(3),S(3),S(3,3),S(3,3),S(3,3,2),S(3,3,2),S(3,3,2),S(3,3,2),S(4),S(4),S(3),S(3),S(3),S(3),one,one,one,one,one,one],
        compiler_params=pltpu.CompilerParams(collective_id=1,has_side_effects=True,vmem_limit_bytes=60*1024*1024),name="life")(vt,tw,hold,shock,brack,coef,const,interest,wage,eff,agg)

def put_out(v,p,h,c,vo,po,ho,co,sem):
    copies=[pltpu.make_async_copy(a,b,sem.at[n]) for n,(a,b) in enumerate(((v,vo),(p,po),(h,ho)))]
    for q in copies:
        q.start()
    for n in range(4):
        co[n]=c[n]
    for q in copies:
        q.wait()

def put_out_call(v,p,h,c):
    vm=pl.BlockSpec(memory_space=pltpu.VMEM); sm=pl.BlockSpec(memory_space=pltpu.SMEM); hb=pl.BlockSpec(memory_space=pltpu.HBM)
    return pl.pallas_call(put_out,out_shape=[jax.ShapeDtypeStruct(a.shape,f32) for a in (v,p,h,c)],in_specs=[vm,vm,vm,sm],out_specs=[hb,hb,hb,sm],
        scratch_shapes=[pltpu.SemaphoreType.DMA((3,))],name="put_out")(v,p,h,c)


def on_device(value_prior,trans_weight,coefficient,constant,interest,wage_level,efficiency,holdings,shocks,brackets,aggregate):
    values_now,policy,final,capital=life_call(value_prior.T,trans_weight,holdings.reshape(64,128),shocks,brackets,coefficient,constant,interest,wage_level,efficiency,aggregate)
    values_now,policy,final,capital=put_out_call(values_now,policy,final,capital)
    return values_now,policy,final.reshape(8192),capital


def solution(mesh):
    finer=Mesh(mesh.devices.reshape(4,4,8,mesh.shape["grid"]),(X,Y,ZC,G))
    in_specs=(P(None,AGENT),P(),P(),P(),P(),P(),P(),P(AGENT),P(None,AGENT),P(None,AGENT),P())
    out_specs=(P(AGENT,G),P(AGENT,G),P(AGENT),P())
    return jax.shard_map(on_device,mesh=finer,in_specs=in_specs,out_specs=out_specs,check_vma=False)
```

```python
import jax
import jax.numpy as jnp
from jax import lax
from jax.experimental import pallas as pl
from jax.experimental.pallas import tpu as pltpu
from jax.sharding import Mesh
from jax.sharding import PartitionSpec as P
MESH=pl.DeviceIdType.MESH
X,Y,ZC,G="agent_0","agent_1","agent_2","grid"
AGENT=(X,Y,ZC)
f32=jnp.float32
i32=jnp.int32
LOG2E=1.4426950408889634
KT=500.0*LOG2E
SP=40.0/15
UN=128

def hat(x,k):
    return jnp.maximum(0.0,1.0-jnp.abs(x-40.0*k/15)/SP)

def rdma(src,dst,ss,rs,**dev):
    return pltpu.make_async_remote_copy(src_ref=src,dst_ref=dst,send_sem=ss,recv_sem=rs,device_id=dev_ids(dev),device_id_type=MESH)
def dev_ids(dev):
    return {dict(x=X,y=Y,z=ZC,g=G)[k]:v for k,v in dev.items()}
def got(ref,sem):
    pltpu.make_async_copy(ref,ref,sem).wait()


CH=((0,8),(8,6),(14,2))

def life(vt_hbm, tw_hbm, hold_hbm, shock_hbm, brack_hbm, coef_ref, const_ref, int_ref, wage_ref, eff_ref, agg_ref,
         v_ref, p_ref, h_ref, cap_ref,
         vt_ref,tw_ref,hold_ref,shock_ref,brack_ref,send,mid,recv,
         pt,kpt,sc,rs,vb,pb,
         pxa,pxb,pxc,y0a,y0b,y0c,z0a,z0b,z0c,yba,ybb,ybc,lk,tt,oh,resa,resb,ri,li,own,pbk,inv,fr_s,hp,hr,pay1,in1,pay2,in2,wt,sl,sd,cl,ctot,cp,c1,c2,c3,
         sin,sa1,ra1,sa2,ra2,sx,rx,sy0,ry0,sz0,rz0,szt,rzt,sya,rya,syb,ryb,sh,rh,s1,r1,s2,r2,sc1,rc1,sc2,rc2,sc3,rc3):
    px=(pxa,pxb,pxc); y0=(y0a,y0b,y0c); z0=(z0a,z0b,z0c); yb=(yba,ybb,ybc); res=(resa,resb)
    x=lax.axis_index(X); y=lax.axis_index(Y); zc=lax.axis_index(ZC); g=lax.axis_index(G)
    inputs=[pltpu.make_async_copy(a,b,sin.at[n]) for n,(a,b) in enumerate(((vt_hbm,vt_ref),(tw_hbm,tw_ref),(hold_hbm,hold_ref),(shock_hbm,shock_ref),(brack_hbm,brack_ref)))]
    for c in inputs:
        c.start()
    bar=pltpu.get_barrier_semaphore()
    me_p=x*4+y
    me_l=zc*2+g
    def plane(d):
        o=lax.rem(me_p+d,16)
        return {X:o//4,Y:lax.rem(o,4)}
    def line(d):
        o=lax.rem(me_l+d,16)
        return {ZC:o//2,G:lax.rem(o,2)}
    def sig(d,_):
        pl.semaphore_signal(bar,inc=1,device_id=plane(d),device_id_type=MESH)
        pl.semaphore_signal(bar,inc=1,device_id=line(d),device_id_type=MESH)
        return 0
    lax.fori_loop(1,16,sig,0)

    lane8=lax.broadcasted_iota(i32,(8,128),1)
    sub8=lax.broadcasted_iota(i32,(8,128),0)
    def expect():
        inputs[0].wait(); inputs[1].wait()
        tw=tw_ref[...]
        tn=tw/jnp.sum(tw,axis=1,keepdims=True)
        blocks=[]
        for k in range(16):
            b=None
            for q in range(4):
                col=(q*4+k//4)*128
                w=vt_ref[:,col:col+128]
                d=(q*32-(k%4)*32)%128
                if d: w=pltpu.roll(w,d,1)
                b=w if b is None else jnp.where(lane8//32==q,w,b)
            blocks.append(b)
        vk=jnp.concatenate(blocks,axis=0)
        bl=lax.dot_general(vk,tn,(((1,),(1,)),((),())),precision=lax.Precision.HIGHEST,preferred_element_type=f32)
        zl=lane8//32
        def per_zone(r):
            return jnp.where(zl==0,r[0],jnp.where(zl==1,r[1],jnp.where(zl==2,r[2],r[3])))
        cf=per_zone(coef_ref); cs=per_zone(const_ref)
        masks=[(lane8//16-sub8)%8==d for d in range(8)]
        for j in range(16):
            fc=jnp.clip(cf*(40.0*j/15)+cs,0.0,40.0)
            acc=None
            for k in range(16):
                w=hat(fc,k)*bl[k*8:k*8+8,:]
                acc=w if acc is None else acc+w
            o=acc
            for d in range(1,8):
                o=jnp.where(masks[d],pltpu.roll(pltpu.roll(acc,8-d,0),16*d,1),o)
            for q in range(8):
                send[(j%4)*2+q%2,(q//2)*4+j//4]=o[q:q+1,:]
    def expect_a():
        def go(d,_):
            o=lax.rem(zc+d,8)
            rdma(send.at[o],mid.at[zc],sa1,ra1,z=o).start()
            return 0
        lax.fori_loop(1,8,go,0)
        mid[zc]=send[zc]
    def expect_b():
        got(mid.at[pl.ds(0,7)],ra1)
        def go(d,_):
            o=lax.rem(me_p+d,16)
            rdma(mid.at[:,o],recv.at[me_p],sa2,ra2,x=o//4,y=lax.rem(o,4)).start()
            return 0
        lax.fori_loop(1,16,go,0)
        recv[me_p]=mid[:,me_p]
    def expect_c():
        got(recv.at[pl.ds(0,15)],ra2)
        for q in range(16):
            rs[q*8:q*8+8,:]=jnp.concatenate([recv[q,n] for n in range(8)],axis=0)*(48.0*LOG2E)

    def pts(A,_):
        for n in range(8):
            t=A*8+n
            j=(64*A+n+8*sub8).astype(f32)
            fr=j/1023.0
            p=40.0*fr*fr
            o=pl.multiple_of(t*8,8)
            pt[pl.ds(o,8),:]=p
            kpt[pl.ds(o,8),:]=p*KT+0.1*KT
        return 0
    k=y*4+zc//2
    eh=lax.rem(zc,2)
    growth=1.0+int_ref[x,k]
    wage=wage_ref[x,k]
    def state(e,_):
        inc=wage*eff_ref[eh*16+e]
        W=[];KW=[]
        for v in range(4):
            i=(lax.broadcasted_iota(i32,(8,128),1)+(128*v+512*g)).astype(f32)
            fr=i/1023.0
            w=(40.0*fr*fr)*growth+inc
            W.append(w);KW.append(w*KT)
        def p1(c,M):
            M=list(M)
            for u in range(UN):
                off=pl.multiple_of((c*UN+u)*8,8)
                P=pt[pl.ds(off,8),:]; KP=kpt[pl.ds(off,8),:]
                Rr=rs[pl.ds(pl.multiple_of((c*(UN//8)+u//8)*8,8),8),:]
                B=jnp.take_along_axis(Rr,jnp.full((8,128),(u%8)*16+e,i32),axis=1,mode="promise_in_bounds")
                D=B-KP
                for v in range(4):
                    cl=jnp.maximum(W[v]-P,0.1)
                    S=lax.log2(cl)*50.0+jnp.minimum(KW[v]+D,B)
                    sc[pl.ds(off,8),128*v:128*v+128]=S
                    M[v]=jnp.maximum(M[v],S)
            return tuple(M)
        M=lax.fori_loop(0,128//UN,p1,tuple(jnp.full((8,128),-1e30,f32) for _ in range(4)))
        def p2(c,acc):
            acc=list(acc)
            for u in range(UN):
                off=pl.multiple_of((c*UN+u)*8,8)
                P=pt[pl.ds(off,8),:]
                for v in range(4):
                    q=jnp.exp2(sc[pl.ds(off,8),128*v:128*v+128]-M[v])
                    acc[v]=acc[v]+q
                    acc[4+v]=acc[4+v]+P*q
            return tuple(acc)
        acc=lax.fori_loop(0,128//UN,p2,tuple(jnp.zeros((8,128),f32) for _ in range(8)))
        for v in range(4):
            m=jnp.max(M[v],axis=0,keepdims=True)
            s=jnp.exp2(M[v]-m)
            tot=jnp.sum(acc[v]*s,axis=0,keepdims=True)
            q=jnp.sum(acc[4+v]*s,axis=0,keepdims=True)
            vb[e,:,128*v:128*v+128]=jnp.broadcast_to((0.02/LOG2E)*m+0.02*jnp.log(tot),(8,128))
            pb[e,:,128*v:128*v+128]=jnp.broadcast_to(q/tot,(8,128))
        return 0
    def bell(a,b):
        lax.fori_loop(a,b,state,0)
    def finish(c):
        a,n=CH[c]
        v_ref[a:a+n,:]=jnp.concatenate([vb[a+q,0:1,:] for q in range(n)],axis=0)
        p=jnp.concatenate([pb[a+q,0:1,:] for q in range(n)],axis=0)
        p_ref[a:a+n,:]=p
        px[c][x]=p

    def send_x(c):
        def go(d,_):
            rdma(px[c].at[x],px[c].at[x],sx.at[c],rx.at[c],x=lax.rem(x+d,4)).start()
            return 0
        lax.fori_loop(1,4,go,0)
    def send_y0(c,w):
        got(px[c].at[pl.ds(0,3)],rx.at[c])
        y0[c][y]=px[c][agg_ref[0]]*w
        def go(d,_):
            rdma(y0[c].at[y],y0[c].at[y],sy0.at[c],ry0.at[c],y=lax.rem(y+d,4)).start()
            return 0
        lax.fori_loop(1,4,go,0)
    def send_z0(c):
        got(y0[c].at[pl.ds(0,3)],ry0.at[c])
        b=y0[c]
        z0[c][zc]=(b[0]+b[1])+(b[2]+b[3])
        def go(d,_):
            rdma(z0[c].at[zc],z0[c].at[zc],sz0.at[c],rz0.at[c],z=lax.rem(zc+d,8)).start()
            return 0
        lax.fori_loop(1,8,go,0)
    def table0(c):
        got(z0[c].at[pl.ds(0,7)],rz0.at[c])
        a,n=CH[c]
        b=z0[c]
        for h in range(2):
            lk[h*16+a:h*16+a+n,:]=(b[h]+b[2+h])+(b[4+h]+b[6+h])
    def send_slot(t,half):
        b=yb[half]
        b[t-1,y,zc]=px[half][agg_ref[t]]
        def go(d,_):
            rdma(b.at[t-1,y,zc],b.at[t-1,y,zc],szt.at[t-1,half],rzt.at[t-1,half],z=lax.rem(zc+d,8)).start()
            return 0
        lax.fori_loop(1,8,go,0)
    up=lax.rem(y+1,4); down=lax.rem(y+3,4)
    def slot_a(t,half):
        b=yb[half]
        got(b.at[t-1,0,pl.ds(0,7)],rzt.at[t-1,half])
        for n,d in ((0,up),(1,down)):
            rdma(b.at[t-1,y],b.at[t-1,y],sya.at[t-1,half,n],rya.at[t-1,half,n],y=d).start()
    def slot_b(t,half):
        b=yb[half]
        got(b.at[t-1,0],rya.at[t-1,half,0])
        rdma(b.at[t-1,down,pl.ds(0,4)],b.at[t-1,down,pl.ds(0,4)],syb.at[t-1,half,0],ryb.at[t-1,half,0],y=up).start()
        got(b.at[t-1,0],rya.at[t-1,half,1])
        rdma(b.at[t-1,up,pl.ds(4,4)],b.at[t-1,up,pl.ds(4,4)],syb.at[t-1,half,1],ryb.at[t-1,half,1],y=down).start()
    def slot_done(t):
        for half in range(3):
            b=yb[half]
            got(b.at[t-1,0,pl.ds(0,4)],ryb.at[t-1,half,0])
            got(b.at[t-1,0,pl.ds(0,4)],ryb.at[t-1,half,1])
    def table(t,cap):
        hs=[hat(cap,q) for q in range(16)]
        for h in range(2):
            for c,(o,n) in enumerate(CH):
                for v in range(4):
                    acc=None
                    for q in range(16):
                        w=hs[q]*yb[c][t-1,q//4,2*(q%4)+h,:,128*v:128*v+128]
                        acc=w if acc is None else acc+w
                    lk[h*16+o:h*16+o+n,128*v:128*v+128]=acc

    def sum_a(t,row):
        pay1[t]=row
        in1[t,me_l]=row
        def go(d,_):
            pltpu.make_async_remote_copy(src_ref=pay1.at[t],dst_ref=in1.at[t,me_l],send_sem=s1.at[t],recv_sem=r1.at[t],device_id=line(d),device_id_type=MESH).start()
            return 0
        lax.fori_loop(1,16,go,0)
    def total(buf,t):
        rows=[buf[t,n] for n in range(16)]
        while len(rows)>1:
            rows=[rows[2*n]+rows[2*n+1] for n in range(len(rows)//2)]
        return rows[0]
    def sum_b(t):
        got(in1.at[t,pl.ds(0,15)],r1.at[t])
        row=total(in1,t)
        pay2[t]=row
        in2[t,me_p]=row
        def go(d,_):
            pltpu.make_async_remote_copy(src_ref=pay2.at[t],dst_ref=in2.at[t,me_p],send_sem=s2.at[t],recv_sem=r2.at[t],device_id=plane(d),device_id_type=MESH).start()
            return 0
        lax.fori_loop(1,16,go,0)
    def sum_c(t):
        got(in2.at[t,pl.ds(0,15)],r2.at[t])
        return total(in2,t)
    def mean_of(t,row):
        cap=jnp.sum(row)/1048576.0
        cap_ref[t]=cap
        return cap

    def index(n,_):
        cols=pl.ds(pl.multiple_of(n*1024,1024),1024)
        b=brack_ref[:,cols]; e=shock_ref[:,cols]
        edge=jnp.logical_and(b==511,g==1)
        mine=(b//512)==g
        r=((b//128)%4)*32+e
        ri[:,cols]=jnp.where(mine,r,jnp.where(edge,96+e,-1))
        li[:,cols]=jnp.where(edge,127,b%128)
        own[:,cols]=jnp.where(edge,0.0,1.0)
        fa=b.astype(f32)/1023.0; fb=(b+1).astype(f32)/1023.0
        lo=40.0*fa*fa; hi=40.0*fb*fb
        pbk[:,cols]=lo
        inv[:,cols]=1.0/(hi-lo)
        return 0
    lane=lax.broadcasted_iota(i32,(32,128),1)
    iota=lax.broadcasted_iota(i32,(128,128),0)
    def hot(t):
        def go(n,_):
            for q in range(8):
                cols=pl.ds(pl.multiple_of(n*1024+q*128,128),128)
                o=jnp.where(jnp.broadcast_to(ri[t:t+1,cols],(128,128))==iota,1.0,0.0).astype(jnp.bfloat16)
                oh[t,0:128,cols]=o
                oh[t,128:256,cols]=o
            return 0
        lax.fori_loop(0,8,go,0)
    def shares(t):
        for n in range(8):
            r8=slice(n*8,n*8+8)
            h=hold_ref[r8,:] if t==0 else hp[t-1,r8,:]+hr[t-1,r8,:]
            for q in range(8):
                cols=slice((n*8+q)*128,(n*8+q)*128+128)
                fr_s[t:t+1,cols]=jnp.clip((h[q:q+1,:]-pbk[t:t+1,cols])*inv[t:t+1,cols],0.0,1.0)
    def gather(t,between=None):
        ls=[lk[:,128*v:128*v+128] for v in range(4)]
        ro=[pltpu.roll(q,127,1) for q in ls]
        ds=[jnp.where(lane==127,ro[v+1],ro[v])-ls[v] for v in range(3)]
        first=jnp.broadcast_to(ls[0][:,0:1],(32,128))
        last=jnp.where(g==1,first,-ls[3])
        ds.append(jnp.where(lane==127,last,ro[3]-ls[3]))
        for o,q in ((0,ls),(128,ds)):
            m=jnp.concatenate(q,axis=0).T
            hi=m.astype(jnp.bfloat16)
            tt[o:o+128,0:128]=hi
            tt[o:o+128,128:256]=(m-hi.astype(f32)).astype(jnp.bfloat16)
        table_now=tt[...]
        for n in range(8):
            if n==3 and between is not None:
                between()
            rb=res[n%2]
            rb[...]=jnp.dot(table_now,oh[t,:,n*1024:n*1024+1024],preferred_element_type=f32)
            for q in range(8):
                cols=slice(n*1024+q*128,n*1024+q*128+128)
                m=jnp.broadcast_to(li[t:t+1,cols],(128,128))==iota
                sl[:,cols]=own[t:t+1,cols]*jnp.sum(jnp.where(m,rb[0:128,q*128:q*128+128],0.0),axis=0,keepdims=True)
                sd[:,cols]=jnp.sum(jnp.where(m,rb[128:256,q*128:q*128+128],0.0),axis=0,keepdims=True)
    def combine(t):
        acc=None
        for n in range(8):
            rows=[]
            for q in range(8):
                cols=slice(n*1024+q*128,n*1024+q*128+128)
                rows.append(sl[:,cols]+fr_s[t:t+1,cols]*sd[:,cols])
            hn=jnp.concatenate(rows,axis=0)
            hp[t,n*8:n*8+8,:]=hn
            acc=hn if acc is None else acc+hn
        rdma(hp.at[t],hr.at[t],sh.at[t],rh.at[t],g=1-g).start()
        return jnp.sum(acc,axis=0,keepdims=True)
    def counts(t):
        acc=None
        for n in range(8):
            for q in range(8):
                cols=slice(n*1024+q*128,n*1024+q*128+128)
                m=jnp.broadcast_to(li[t:t+1,cols],(128,128))==iota
                wt[0:128,q*128:q*128+128]=jnp.where(m,jnp.broadcast_to(own[t:t+1,cols],(128,128)),0.0).astype(jnp.bfloat16)
            d=lax.dot_general(oh[t,0:128,n*1024:n*1024+1024],wt[0:128,:],(((1,),(1,)),((),())),preferred_element_type=f32)
            acc=d if acc is None else acc+d
        cl[...]=acc
    def weights(t,between=None):
        acc=None
        for n in range(8):
            if n==3 and between is not None:
                between()
            for q in range(8):
                cols=slice(n*1024+q*128,n*1024+q*128+128)
                m=jnp.broadcast_to(li[t:t+1,cols],(128,128))==iota
                f=fr_s[t:t+1,cols]
                hi=f.astype(jnp.bfloat16).astype(f32)
                wt[0:128,q*128:q*128+128]=jnp.where(m,jnp.broadcast_to(hi,(128,128)),0.0).astype(jnp.bfloat16)
                wt[128:256,q*128:q*128+128]=jnp.where(m,jnp.broadcast_to(f-hi,(128,128)),0.0).astype(jnp.bfloat16)
            d=lax.dot_general(oh[t,0:128,n*1024:n*1024+1024],wt[...],(((1,),(1,)),((),())),preferred_element_type=f32)
            acc=d if acc is None else acc+d
        cd=acc[:,0:128]+acc[:,128:256]
        cs=[cd[32*v:32*v+32,:] for v in range(4)]
        ro=[pltpu.roll(q,1,1) for q in cs]
        for v in range(4):
            if v==3:
                inner=jnp.where(lane==127,0.0,cs[3])
                ctot_v=cl[96:128,:]-inner
                ctot_v=ctot_v-jnp.where(jnp.logical_and(lane==127,g==0),cs[3],0.0)
            else:
                ctot_v=cl[32*v:32*v+32,:]-cs[v]
            prev=ro[v-1] if v else jnp.where(g==1,ro[3],jnp.zeros_like(ro[3]))
            ctot[:,128*v:128*v+128]=ctot_v+jnp.where(lane==0,prev,ro[v])
    lane1=lax.broadcasted_iota(i32,(1,128),1)
    def moments(t,row):
        out=jnp.where(lane1==16,jnp.sum(row,axis=1,keepdims=True),0.0)
        for q in range(16):
            m=None
            for c,(o,n) in enumerate(CH):
                acc=None
                for h in range(2):
                    for v in range(4):
                        w=ctot[h*16+o:h*16+o+n,128*v:128*v+128]*yb[c][t-1,q//4,2*(q%4)+h,:,128*v:128*v+128]
                        acc=w if acc is None else acc+w
                acc=jnp.sum(acc,axis=0,keepdims=True)
                m=acc if m is None else m+acc
            m=jnp.sum(m,axis=1,keepdims=True)
            out=jnp.where(lane1==q,m,out)
        return out

    def spread_a():
        for q in range(8):
            o=(q%2)*16+(q//2)*4
            cp[q]=ctot[o:o+4,:]
        c1[zc]=cp[zc]
        def go(d,_):
            o=lax.rem(zc+d,8)
            rdma(cp.at[o],c1.at[zc],sc1,rc1,z=o).start()
            return 0
        lax.fori_loop(1,8,go,0)
    def added(b,n):
        rows=[b[q] for q in range(n)]
        while len(rows)>1:
            rows=[rows[2*q]+rows[2*q+1] for q in range(len(rows)//2)]
        return rows[0]
    def spread_b():
        got(c1.at[pl.ds(0,7)],rc1)
        c2[me_p]=added(c1,8)
        def go(d,_):
            o=lax.rem(me_p+d,16)
            rdma(c2.at[me_p],c2.at[me_p],sc2,rc2,x=o//4,y=lax.rem(o,4)).start()
            return 0
        lax.fori_loop(1,16,go,0)
    def spread_c():
        got(c2.at[pl.ds(0,15)],rc2)
        c3[zc//2]=added(c2,16)
        def go(d,_):
            rdma(c3.at[zc//2],c3.at[zc//2],sc3,rc3,z=lax.rem(zc+2*d,8)).start()
            return 0
        lax.fori_loop(1,4,go,0)
    def first_mean(w):
        got(c3.at[pl.ds(0,3)],rc3)
        acc=None
        for q in range(4):
            w4=c3[q]*p_ref[q*4:q*4+4,:]
            acc=w4 if acc is None else acc+w4
        row=jnp.sum(acc,axis=0,keepdims=True)
        row=(row[:,0:128]+row[:,128:256])+(row[:,256:384]+row[:,384:512])
        return row*(w*jnp.where(agg_ref[0]==x,1.0,0.0))

    expect()
    pl.semaphore_wait(bar,30)
    expect_a()
    for c in inputs[2:]:
        c.wait()
    h0=jnp.zeros((8,128),f32)
    for n in range(4):
        h0=h0+hold_ref[pl.ds(pl.multiple_of(g*32+n*8,8),8),:]
    sum_a(0,jnp.sum(h0,axis=0,keepdims=True))
    lax.fori_loop(0,8,index,0)
    shares(0)
    hot(0)
    lax.fori_loop(0,16,pts,0)
    expect_b()
    counts(0)
    sum_b(0)
    weights(0)
    spread_a()
    expect_c()
    bell(0,4)
    row=sum_c(0)
    cap=mean_of(0,row)
    kf=k.astype(f32)
    w0=jnp.maximum(0.0,1.0-jnp.abs(cap-40.0*kf/15)/SP)
    spread_b()
    bell(4,8)
    finish(0)
    send_x(0)
    spread_c()
    bell(8,11)
    send_y0(0,w0)
    send_slot(1,0)
    send_slot(2,0)
    bell(11,14)
    finish(1)
    send_x(1)
    send_z0(0)
    bell(14,16)
    finish(2)
    send_x(2)
    sum_a(1,first_mean(w0))
    send_y0(1,w0)
    send_slot(1,1)
    hot(1)
    send_y0(2,w0)
    send_slot(1,2)
    send_z0(1)
    slot_a(1,0)
    send_z0(2)
    sum_b(1)
    send_slot(2,1)
    send_slot(2,2)
    for n in range(3):
        send_slot(3,n)
    slot_a(2,0)
    hot(2)
    slot_a(1,1)
    slot_a(1,2)
    slot_b(1,0)
    table0(0)
    table0(1)
    table0(2)
    gather(0)
    combine(0)
    counts(2)
    slot_b(1,1)
    slot_b(1,2)
    slot_a(2,1)
    slot_a(2,2)
    slot_b(2,0)
    cap=mean_of(1,sum_c(1))
    slot_done(1)
    table(1,cap)
    gather(1)
    got(hr.at[0],rh.at[0])
    shares(1)
    row=combine(1)
    got(hr.at[1],rh.at[1])
    shares(2)
    slot_b(2,1)
    slot_b(2,2)
    def later2():
        for n in range(3):
            slot_a(3,n)
    weights(2,later2)
    slot_done(2)
    sum_a(2,moments(2,row))
    hot(3)
    sum_b(2)
    for n in range(3):
        slot_b(3,n)
    row=sum_c(2)
    cap=jnp.sum(jnp.where(lane1==16,row,0.0))/1048576.0
    cap_ref[2]=cap
    table(2,cap)
    qs=lane1.astype(f32)*40.0/15
    cap3=jnp.sum(jnp.where(lane1<16,jnp.maximum(0.0,1.0-jnp.abs(cap-qs)/SP)*row,0.0))/1048576.0
    cap_ref[3]=cap3
    gather(2)
    combine(2)
    slot_done(3)
    table(3,cap3)
    gather(3)
    got(hr.at[2],rh.at[2])
    shares(3)
    combine(3)
    got(mid.at[pl.ds(0,7)],sa1)
    got(recv.at[pl.ds(0,15)],sa2)
    got(c1.at[pl.ds(0,7)],sc1)
    got(c2.at[pl.ds(0,15)],sc2)
    got(c3.at[pl.ds(0,3)],sc3)
    for c in range(3):
        got(px[c].at[pl.ds(0,3)],sx.at[c])
        got(y0[c].at[pl.ds(0,3)],sy0.at[c])
        got(z0[c].at[pl.ds(0,7)],sz0.at[c])
    for t in range(3):
        for half in range(3):
            b=yb[half]
            got(b.at[t,0,pl.ds(0,7)],szt.at[t,half])
            for n in range(2):
                got(b.at[t,0],sya.at[t,half,n])
                got(b.at[t,0,pl.ds(0,4)],syb.at[t,half,n])
    for t in range(4):
        got(hp.at[t],sh.at[t])
    for t in range(3):
        got(in1.at[t,pl.ds(0,15)],s1.at[t])
        got(in2.at[t,pl.ds(0,15)],s2.at[t])
    got(hr.at[3],rh.at[3])
    h_ref[...]=hp[3]+hr[3]

def life_call(vt,tw,hold,shock,brack,coef,const,interest,wage,eff,agg):
    vm=pl.BlockSpec(memory_space=pltpu.VMEM); sm=pl.BlockSpec(memory_space=pltpu.SMEM); hb=pl.BlockSpec(memory_space=pltpu.HBM)
    V=lambda *s: pltpu.VMEM(s,f32)
    B=lambda *s: pltpu.VMEM(s,jnp.bfloat16)
    I=lambda *s: pltpu.VMEM(s,i32)
    S=lambda *s: pltpu.SemaphoreType.DMA(s)
    one=pltpu.SemaphoreType.DMA
    return pl.pallas_call(life,
        out_shape=[jax.ShapeDtypeStruct((16,512),f32),jax.ShapeDtypeStruct((16,512),f32),jax.ShapeDtypeStruct((64,128),f32),jax.ShapeDtypeStruct((4,),f32)],
        in_specs=[hb]*5+[sm]*6,out_specs=[vm,vm,vm,sm],
        scratch_shapes=[V(8,2048),V(128,128),V(64,128),I(4,8192),I(4,8192),V(8,16,1,128),V(8,16,1,128),V(16,8,1,128),
            V(1024,128),V(1024,128),V(1024,512),V(128,128),V(16,8,512),V(16,8,512),
            V(4,8,512),V(4,6,512),V(4,2,512),V(4,8,512),V(4,6,512),V(4,2,512),V(8,8,512),V(8,6,512),V(8,2,512),
            V(3,4,8,8,512),V(3,4,8,6,512),V(3,4,8,2,512),V(32,512),B(256,256),B(4,256,8192),V(256,1024),V(256,1024),
            I(4,8192),I(4,8192),V(4,8192),V(4,8192),V(4,8192),V(4,8192),V(4,64,128),V(4,64,128),V(3,1,128),V(3,16,1,128),V(3,1,128),V(3,16,1,128),
            B(256,1024),V(1,8192),V(1,8192),V(128,128),V(32,512),V(8,4,512),V(8,4,512),V(16,4,512),V(4,4,512),
            S(5),one,one,one,one,S(3),S(3),S(3),S(3),S(3),S(3),S(3,3),S(3,3),S(3,3,2),S(3,3,2),S(3,3,2),S(3,3,2),S(4),S(4),S(3),S(3),S(3),S(3),one,one,one,one,one,one],
        compiler_params=pltpu.CompilerParams(collective_id=1,has_side_effects=True,vmem_limit_bytes=60*1024*1024),name="life")(vt,tw,hold,shock,brack,coef,const,interest,wage,eff,agg)

def put_out(v,p,h,c,vo,po,ho,co):
    for n in range(4):
        co[n]=c[n]
    vo[...]=v[...]
    po[...]=p[...]
    ho[...]=h[...]

def put_out_call(v,p,h,c):
    vm=pl.BlockSpec(memory_space=pltpu.VMEM); sm=pl.BlockSpec(memory_space=pltpu.SMEM)
    return pl.pallas_call(put_out,out_shape=[jax.ShapeDtypeStruct(a.shape,f32) for a in (v,p,h,c)],in_specs=[vm,vm,vm,sm],out_specs=[vm,vm,vm,sm],name="put_out")(v,p,h,c)


def on_device(value_prior,trans_weight,coefficient,constant,interest,wage_level,efficiency,holdings,shocks,brackets,aggregate):
    values_now,policy,final,capital=life_call(value_prior.T,trans_weight,holdings.reshape(64,128),shocks,brackets,coefficient,constant,interest,wage_level,efficiency,aggregate)
    values_now,policy,final,capital=put_out_call(values_now,policy,final,capital)
    return values_now,policy,final.reshape(8192),capital


def solution(mesh):
    finer=Mesh(mesh.devices.reshape(4,4,8,mesh.shape["grid"]),(X,Y,ZC,G))
    in_specs=(P(None,AGENT),P(),P(),P(),P(),P(),P(),P(AGENT),P(None,AGENT),P(None,AGENT),P())
    out_specs=(P(AGENT,G),P(AGENT,G),P(AGENT),P())
    return jax.shard_map(on_device,mesh=finer,in_specs=in_specs,out_specs=out_specs,check_vma=False)
```
